32 devices in a mesh: groups: 2 (over x), ty: 8 (over z, y), tx: 2 (over core).
Axes of the slice: x: 2, y: 2, z: 4, core: 2. Of those that a mesh axis runs over, the one named last changes fastest.
Arguments:
- fields: bfloat16 [6, 2048, 1024], P(None, ('groups', 'ty'), 'tx'), parts along dimension 1, may hold values from -8 to 8
- weights: bfloat16 [2048, 1024], P(('groups', 'ty'), 'tx'), parts along dimension 0, may hold values from 0.049804688 to 0.94921875
- source_tile: int32 [16, 8, 2], P(('groups', 'ty'), 'tx'), parts along dimension 0, may hold values from 0 to 15, as said below
- source_block: int32 [16, 8, 2], P(('groups', 'ty'), 'tx'), parts along dimension 0, may hold values from 0 to 3
- coupling: bfloat16 [6, 6], replicated, may hold values from -2.5 to 2.5
- driver: float32 [6, 128, 128], replicated, may hold values from -48 to 48
- relaxation: float32 [6, 128, 128], replicated, may hold values from 0.05 to 0.6
Outputs:
- nudged: float32 [6, 2048, 1024], P(None, ('groups', 'ty'), 'tx'), parts along dimension 1
The draws below stay inside these ranges and needn't reach their ends.
There are 2 independent parts, one for each index of `groups`. The reference program is written for one: setup_inputs(seed, part) draws one part's arguments, and reference() takes and returns one part's arrays. A program takes and returns all parts, laid end to end along the dimension named above; an argument that names none is the same for every part. Nothing has to cross between parts.
Inputs may be any that keep to these rules, and one draw needn't show every extreme that they name: `source_tile`: the two sources of a block lie in the same block row, the second one block column east of the first (wrapping around the domain). Among the 8 requests of one tile, no tile row of owners is named more than 4 times, and in every tile some owner tile is named exactly 4 times.
All inputs are finite; a program needn't handle non-finite values.
Results may differ from the reference program's by a relative error of at most 0.0003.
Values may be sent and summed in bfloat16 or wider, within the bound.
A program may use at most 128 MiB of HBM per device.

```python
import math
import jax
import jax.numpy as jnp
from jax import lax

FIELDS = 6
BS = 128
KSRC = 2
KMAX = 64
MODES = 128
TH = 128
TW = 512
BX = 4
NY = 1024
NX = 1024
NBY = 8
NBX = 8
N_TY = 8
N_TX = 2


def request_table(key):
    base = jax.random.fold_in(key, 7303)
    key_wy, key_wx, key_pair, key_far = jax.random.split(base, 4)
    wind_y = jax.random.randint(key_wy, (N_TY, N_TX), -3, 4)
    wind_x = jax.random.randint(key_wx, (N_TY, N_TX), -6, 7)
    far_row = jax.random.randint(jax.random.fold_in(key_far, 1), (), 0, N_TY)
    far_col = jax.random.randint(jax.random.fold_in(key_far, 2), (), 0, N_TX)
    tile_row = jnp.arange(N_TY, dtype=jnp.int32)[:, None, None]
    tile_col = jnp.arange(N_TX, dtype=jnp.int32)[None, :, None]
    is_far = (tile_row[..., 0] == far_row) & (tile_col[..., 0] == far_col)
    wind_y = jnp.where(is_far, N_TY // 2, wind_y)
    wind_x = jnp.where(is_far, 0, wind_x)
    offset = 2 * jax.random.randint(key_pair, (N_TY, N_TX), 0, BX // 2)
    column = jnp.arange(BX, dtype=jnp.int32)
    pair_row = (column[None, None, :] + offset[..., None]) % BX // 2 - BX // 4
    source_row = (tile_row + wind_y[..., None] + pair_row) % NBY
    first_col = (tile_col * BX + column[None, None, :] + wind_x[..., None]) % NBX
    both_cols = jnp.stack([first_col, (first_col + 1) % NBX], axis=-1)
    both_rows = jnp.broadcast_to(source_row[..., None], both_cols.shape)
    owners = both_rows * N_TX + both_cols // BX
    blocks = both_cols % BX
    return (owners.reshape(NBY, NBX, KSRC).astype(jnp.int32), blocks.reshape(NBY, NBX, KSRC).astype(jnp.int32))


def draw_source_tile(key, part):
    return request_table(key)[0]


def draw_source_block(key, part):
    return request_table(key)[1]


def draw_fields(key, part):
    key_rough, key_scale, key_ky, key_kx, key_py, key_px, key_amp = jax.random.split(jax.random.fold_in(key, 911), 7)
    spread = jnp.exp(jax.random.uniform(key_scale, (FIELDS, NY, NX), jnp.float32, -0.7, 0.7))
    rough = jnp.clip(jax.random.normal(key_rough, (FIELDS, NY, NX), jnp.float32), -3.0, 3.0) * spread
    wave_y = jax.random.randint(key_ky, (FIELDS, 6), 0, 9).astype(jnp.float32)
    wave_x = jax.random.randint(key_kx, (FIELDS, 6), 0, 9).astype(jnp.float32)
    phase_y = jax.random.uniform(key_py, (FIELDS, 6), jnp.float32, -math.pi, math.pi)
    phase_x = jax.random.uniform(key_px, (FIELDS, 6), jnp.float32, -math.pi, math.pi)
    amplitude = jax.random.uniform(key_amp, (FIELDS, 6), jnp.float32, 0.2, 0.5)
    rows_f = jnp.arange(NY, dtype=jnp.float32)
    cols_f = jnp.arange(NX, dtype=jnp.float32)
    angle_y = 2.0 * math.pi * wave_y[..., None] * rows_f / NY + phase_y[..., None]
    angle_x = 2.0 * math.pi * wave_x[..., None] * cols_f / NX + phase_x[..., None]
    smooth = jnp.einsum('fwy,fwx->fyx', amplitude[..., None] * jnp.cos(angle_y), jnp.cos(angle_x))
    smooth = smooth - jnp.einsum('fwy,fwx->fyx', amplitude[..., None] * jnp.sin(angle_y), jnp.sin(angle_x))
    return jnp.clip(rough + smooth, -8.0, 8.0).astype(jnp.bfloat16)


def steps_of(key, shape, shards, low, largest):
    gain, own = 1.0, jax.random.fold_in(key, 6)
    for dim, shards_of in shards:
        draws = jnp.exp(jax.random.uniform(jax.random.fold_in(own, dim), (shards_of,), jnp.float32, low / len(shards), largest / len(shards)))
        gain = gain * jnp.repeat(draws, shape[dim] // shards_of).reshape([-1 if axis == dim else 1 for axis in range(len(shape))])
    return gain


def gaussian(key, shape, width, limit, kind=jnp.bfloat16):
    array = jax.random.normal(key, shape, jnp.float32) * width
    return jnp.minimum(jnp.maximum(array, -limit), limit).astype(kind)


def setup_inputs(seed: int = 0, part: int = 0) -> dict:
    key_of = jax.random.split(jax.random.key(seed), 8)
    part_keys = jax.random.split(jax.random.fold_in(key_of[7], part), 8)
    fields = draw_fields(jax.random.fold_in(jax.random.fold_in(key_of[7], part), 71), part)
    weights = jnp.clip(0.049804688 + 0.89941406 * jax.random.uniform(part_keys[1], (NY, NX), jnp.float32) ** steps_of(part_keys[1], (NY, NX), ((0, 8), (1, 2)), -0.2, 0.2), 0.049804688, 0.94921875).astype(jnp.bfloat16)
    source_tile = draw_source_tile(jax.random.fold_in(jax.random.fold_in(key_of[7], part), 71), part)
    source_block = draw_source_block(jax.random.fold_in(jax.random.fold_in(key_of[7], part), 71), part)
    coupling = gaussian(key_of[4], (FIELDS, FIELDS), FIELDS ** -0.5, 2.5)
    driver = gaussian(key_of[5], (FIELDS, MODES, MODES), 8.0, 48.0, jnp.float32)
    relaxation = jnp.clip(jax.random.uniform(key_of[6], (FIELDS, MODES, MODES), jnp.float32, 0.05, 0.6), 0.05, 0.6)
    return {"fields": fields, "weights": weights, "source_tile": source_tile, "source_block": source_block, "coupling": coupling, "driver": driver, "relaxation": relaxation}


def wave_basis(offset, extent, period):
    position = offset + jnp.arange(extent, dtype=jnp.int32)
    mode_index = jnp.arange(KMAX, dtype=jnp.int32)
    cos_phase = position[:, None] * mode_index[None, :] % period
    sin_phase = position[:, None] * (mode_index[None, :] + 1) % period
    norming = jnp.where(mode_index == 0, math.sqrt(1.0 / period), math.sqrt(2.0 / period)).astype(jnp.float32)
    cos_part = jnp.cos(2.0 * math.pi * cos_phase.astype(jnp.float32) / period) * norming[None, :]
    sin_part = jnp.sin(2.0 * math.pi * sin_phase.astype(jnp.float32) / period) * math.sqrt(2.0 / period)
    return jnp.concatenate([cos_part, sin_part], axis=1).astype(jnp.float32)

def reference(fields, weights, source_tile, source_block, coupling, driver, relaxation):
    highest = lax.Precision.HIGHEST

    def fetch_block(tile_id, block_id):
        row_start = tile_id // N_TX * TH + block_id // BX * BS
        col_start = tile_id % N_TX * TW + block_id % BX * BS
        return lax.dynamic_slice(fields, (jnp.int32(0), row_start.astype(jnp.int32), col_start.astype(jnp.int32)), (FIELDS, BS, BS))

    def one_row(block_row):
        sources = jax.vmap(jax.vmap(fetch_block))(source_tile[block_row], source_block[block_row])
        row_weights = lax.dynamic_slice_in_dim(weights, (block_row * BS).astype(jnp.int32), BS, 0)
        row_weights = row_weights.reshape(BS, NBX, BS).transpose(1, 0, 2).astype(jnp.float32)
        first = sources[:, 0].astype(jnp.float32)
        second = sources[:, 1].astype(jnp.float32)
        blended = row_weights[:, None] * first + (1.0 - row_weights)[:, None] * second
        return blended.transpose(1, 2, 0, 3).reshape(FIELDS, BS, NX)
    upstream_rows = lax.map(one_row, jnp.arange(NBY, dtype=jnp.int32))
    interpolated = upstream_rows.transpose(1, 0, 2, 3).reshape(FIELDS, NY, NX)
    tendency = jnp.einsum('gf,fyx->gyx', coupling.astype(jnp.float32), fields.astype(jnp.float32), precision=highest)
    upstream = interpolated + tendency
    row_basis = wave_basis(0, NY, NY)
    col_basis = wave_basis(0, NX, NX)
    col_modes = jnp.einsum('fyx,xn->fyn', upstream, col_basis, precision=highest)
    coefficients = jnp.einsum('ym,fyn->fmn', row_basis, col_modes, precision=highest)
    nudge_term = relaxation * (driver - coefficients)
    row_recon = jnp.einsum('ym,fmn->fyn', row_basis, nudge_term, precision=highest)
    correction = jnp.einsum('fyn,xn->fyx', row_recon, col_basis, precision=highest)
    return upstream + correction
```

```python
import functools
import math

import jax
import jax.numpy as jnp
import numpy as np
from jax import lax
from jax.experimental import pallas as pl
from jax.experimental.pallas import tpu as pltpu
from jax.sharding import PartitionSpec as P

BS = 128
KMAX = 64
GROUP = 2
MESH = pl.DeviceIdType.MESH
HI = lax.Precision.HIGHEST


def wave_table(period):
    position = np.arange(period, dtype=np.int64)[:, None]
    mode = np.arange(KMAX, dtype=np.int64)[None, :]
    norming = np.where(mode == 0, math.sqrt(1.0 / period), math.sqrt(2.0 / period))
    cos_part = np.cos(2.0 * math.pi * (position * mode % period) / period) * norming
    sin_part = np.sin(2.0 * math.pi * (position * (mode + 1) % period) / period) * math.sqrt(2.0 / period)
    return np.concatenate([cos_part, sin_part], axis=1).astype(np.float32)


def two_lines(mesh):
    devices = np.asarray(mesh.devices)
    axis = list(mesh.axis_names).index("ty")
    line = np.moveaxis(devices, axis, 0).reshape(devices.shape[axis], -1)[:, 0]
    coords = [getattr(d, "coords", None) for d in line]
    if any(c is None for c in coords) or len(line) % 2:
        return False
    varying = [k for k in range(len(coords[0])) if len({c[k] for c in coords}) > 1]
    return len(varying) > 1


def ring_kernel(
    n_ty, n_tx, snake,
    fields, weights_hbm, picks, coupling, driver_hbm, relaxation_hbm, row_tab, row_tab_t, col_tab,
    out, *scratch,
):
    n_fields, rows, cols = fields.shape
    gathered = scratch[:n_fields]
    n_groups = n_fields // GROUP
    (modes, swapped, chip_sums, rs_bufs, sums, ag_bufs) = (
        scratch[n_fields + k * n_groups : n_fields + (k + 1) * n_groups] for k in range(6))
    (row_b, row_bt, col_b, weights, driver, relaxation, tab_sem, own_sem, ring_send, ring_recv, mate_send, mate_recv,
     rs_send, rs_recv, ag_send, ag_recv, swap_send, swap_recv, back_send, back_recv) = scratch[n_fields + 6 * n_groups :]
    per_tile = cols // BS
    ty = lax.axis_index("ty")
    tx = lax.axis_index("tx")
    mate = 1 - tx
    depth = n_ty // 2

    def ring_to_ty(pos):
        pos = (pos + n_ty) % n_ty
        if not snake:
            return pos
        return jnp.where(pos < n_ty // 2, 2 * pos, 2 * (n_ty - 1 - pos) + 1)

    ring = jnp.where(ty % 2 == 0, ty // 2, n_ty - 1 - ty // 2) if snake else ty
    toward = (ring_to_ty(ring + 1), ring_to_ty(ring - 1))

    tabs = [
        pltpu.make_async_copy(row_tab.at[pl.ds(ty * rows, rows), :], row_b, tab_sem.at[0]),
        pltpu.make_async_copy(row_tab_t.at[:, pl.ds(pl.multiple_of(ty * rows, 128), rows)], row_bt, tab_sem.at[1]),
        pltpu.make_async_copy(col_tab.at[pl.ds(tx * cols, cols), :], col_b, tab_sem.at[2]),
        pltpu.make_async_copy(weights_hbm, weights, tab_sem.at[3]),
        pltpu.make_async_copy(driver_hbm, driver, tab_sem.at[4]),
        pltpu.make_async_copy(relaxation_hbm, relaxation, tab_sem.at[5]),
    ]

    def tile_of(f, col, row, part=None):
        first, count = (col * n_ty + row) * per_tile, per_tile
        if part is not None:
            count = per_tile // 2
            first = first + part * count
        return gathered[f].at[pl.ds(first, count)]

    def column_of(f, col):
        return gathered[f].at[pl.ds(col * n_ty * per_tile, n_ty * per_tile)]

    barrier = pltpu.get_barrier_semaphore()
    pl.semaphore_signal(barrier, inc=1, device_id={"tx": mate}, device_id_type=MESH)
    for k in range(1, n_ty):
        pl.semaphore_signal(barrier, inc=1, device_id={"ty": (ty + k) % n_ty}, device_id_type=MESH)
    here = (tx * n_ty + ty) * per_tile

    own = [
        pltpu.make_async_copy(fields.at[f, :, pl.ds(b * BS, BS)], gathered[f].at[here + b], own_sem.at[f, b])
        for f in range(n_fields)
        for b in range(per_tile)
    ]
    for copy in own + tabs:
        copy.start()
    pl.semaphore_wait(barrier, n_ty)
    for copy in own:
        copy.wait()

    def to_mate(f, ref):
        return pltpu.make_async_remote_copy(
            src_ref=ref, dst_ref=ref, send_sem=mate_send.at[f], recv_sem=mate_recv.at[f],
            device_id={"tx": mate}, device_id_type=MESH)

    def sign(way):
        return 1 if way == 0 else -1

    def travels(way, h, d):
        return d < depth - 1 or (d == depth - 1 and h == way)

    def ring_copy(f, way, h, d):
        ref = tile_of(f, tx, ring_to_ty(ring - sign(way) * d), h)
        return pltpu.make_async_remote_copy(
            src_ref=ref, dst_ref=ref,
            send_sem=ring_send.at[f], recv_sem=ring_recv.at[f, way, h, d],
            device_id={"ty": toward[way]}, device_id_type=MESH)

    def arrived(f, way, h, d):
        ref = tile_of(f, tx, ring_to_ty(ring - sign(way) * (d + 1)), h)
        pltpu.make_async_remote_copy(
            src_ref=ref, dst_ref=ref, send_sem=ring_send.at[f], recv_sem=ring_recv.at[f, way, h, d],
            device_id={"ty": toward[way]}, device_id_type=MESH).wait_recv()
        return ref

    def stage(g, d):
        for f in range(g * GROUP, (g + 1) * GROUP):
            for h in range(2):
                for way in range(2):
                    came = d > 0 and travels(way, h, d - 1)
                    if came:
                        got = arrived(f, way, h, d - 1)
                    if travels(way, h, d):
                        ring_copy(f, way, h, d).start()
                    if came:
                        to_mate(f, got).start()
            if d == 0:
                to_mate(f, tile_of(f, tx, ty)).start()

    def tendency(g):
        for f in range(g * GROUP, (g + 1) * GROUP):
            for b in range(per_tile):
                span = slice(b * BS, (b + 1) * BS)
                total = coupling[f : f + 1, 0:1].astype(jnp.float32) * gathered[0][here + b].astype(jnp.float32)
                for k in range(1, n_fields):
                    total = total + coupling[f : f + 1, k : k + 1].astype(jnp.float32) * gathered[k][here + b].astype(jnp.float32)
                out[f, :, span] = total

    def upstream(g):
        for f in range(g * GROUP, (g + 1) * GROUP):
            to_mate(f, column_of(f, mate)).wait_recv()
            for j in range(per_tile):
                span = slice(j * BS, (j + 1) * BS)

                first = gathered[f][picks[0, j]].astype(jnp.float32)
                second = gathered[f][picks[1, j]].astype(jnp.float32)
                w = weights[:, span].astype(jnp.float32)
                out[f, :, span] = out[f, :, span] + (w * first + (1.0 - w) * second)
            col_modes = jnp.zeros((rows, 128), jnp.float32)
            for start in range(0, cols, 2 * BS):
                span = slice(start, start + 2 * BS)
                col_modes += jnp.dot(out[f, :, span], col_b[span, :], precision=HI, preferred_element_type=jnp.float32)
            part = jnp.dot(row_bt[...], col_modes, precision=HI, preferred_element_type=jnp.float32)
            modes[g][pl.ds((f - g * GROUP) * 128, 128), :] = part
        swap_copy(g).start()

    half = GROUP * 128 // n_tx
    span_rows = half // n_ty

    def half_copy(src, dst, send, recv):
        return pltpu.make_async_remote_copy(
            src_ref=src, dst_ref=dst, send_sem=send, recv_sem=recv, device_id={"tx": mate}, device_id_type=MESH)

    def swap_copy(g):
        src = modes[g].at[pl.ds(pl.multiple_of(mate * half, 8), half), :]
        return half_copy(src, swapped[g], swap_send.at[g], swap_recv.at[g])

    def back_copy(g):
        ref = ag_bufs[g].at[pl.ds(pl.multiple_of(tx * half, 8), half), :]
        return half_copy(ref, ref, back_send.at[g], back_recv.at[g])

    def rs_copy(g, k):
        there = (ty + k) % n_ty
        return pltpu.make_async_remote_copy(
            src_ref=chip_sums[g].at[pl.ds(pl.multiple_of(there * span_rows, 8), span_rows), :], dst_ref=rs_bufs[g].at[k - 1],
            send_sem=rs_send.at[g], recv_sem=rs_recv.at[g], device_id={"ty": there}, device_id_type=MESH)

    def ag_copy(g, k):
        there = (ty + k) % n_ty
        return pltpu.make_async_remote_copy(
            src_ref=sums[g], dst_ref=ag_bufs[g].at[pl.ds(pl.multiple_of(tx * half + ty * span_rows, 8), span_rows), :],
            send_sem=ag_send.at[g], recv_sem=ag_recv.at[g], device_id={"ty": there}, device_id_type=MESH)

    def scatter(g):
        swap_copy(g).wait_recv()
        chip_sums[g][...] = modes[g][pl.ds(pl.multiple_of(tx * half, 8), half), :] + swapped[g][...]
        for k in range(1, n_ty):
            rs_copy(g, k).start()

    def reduce(g):
        whole = rs_bufs[g]
        half_copy(whole, whole, rs_send.at[g], rs_recv.at[g]).wait_recv()
        mine = chip_sums[g][pl.ds(pl.multiple_of(ty * span_rows, 8), span_rows), :]
        total = mine + jnp.sum(rs_bufs[g][...], axis=0)
        sums[g][...] = total
        for k in range(1, n_ty):
            ag_copy(g, k).start()
        ag_bufs[g][pl.ds(pl.multiple_of(tx * half + ty * span_rows, 8), span_rows), :] = total

    def hand_back(g):
        whole = rs_bufs[g]
        half_copy(whole, whole, ag_send.at[g], ag_recv.at[g]).wait_recv()
        back_copy(g).start()

    def nudge(g):
        ref = ag_bufs[g].at[pl.ds(pl.multiple_of(mate * half, 8), half), :]
        half_copy(ref, ref, back_send.at[g], back_recv.at[g]).wait_recv()
        for f in range(g * GROUP, (g + 1) * GROUP):
            coef = ag_bufs[g][pl.ds((f - g * GROUP) * 128, 128), :]
            term = relaxation[f] * (driver[f] - coef)
            recon = jnp.dot(row_b[...], term, precision=HI, preferred_element_type=jnp.float32)
            for start in range(0, cols, 2 * BS):
                span = slice(start, start + 2 * BS)
                out[f, :, span] += lax.dot_general(
                    recon, col_b[span, :], (((1,), (1,)), ((), ())), precision=HI, preferred_element_type=jnp.float32)

    stage(0, 0)
    for g in range(n_groups):
        tendency(g)
    for copy in tabs:
        copy.wait()
    end = n_groups - 1
    for g in range(end):
        behind = [upstream, scatter, reduce] if g > 0 else []
        for d in range(1, depth):
            stage(g, d)
            if behind:
                behind.pop(0)(g - 1)
        stage(g + 1, 0)
        stage(g, depth)
        if g > 0:
            for step in behind + [hand_back, nudge]:
                step(g - 1)
    for d in range(1, depth):
        stage(end, d)
        if d == 1:
            upstream(end - 1)
    scatter(end - 1)
    stage(end, depth)
    reduce(end - 1)
    upstream(end)
    scatter(end)
    hand_back(end - 1)
    reduce(end)
    nudge(end - 1)
    hand_back(end)
    nudge(end)

    for f in range(n_fields):
        sent = gathered[f].at[pl.ds(0, (n_ty - 1) * per_tile)]
        pltpu.make_async_remote_copy(
            src_ref=sent, dst_ref=sent, send_sem=ring_send.at[f], recv_sem=ring_recv.at[f, 0, 0, 0],
            device_id={"ty": toward[0]}, device_id_type=MESH).wait_send()
        to_mate(f, column_of(f, tx)).wait_send()
    for g in range(n_groups):
        swap_copy(g).wait_send()
        back_copy(g).wait_send()
        whole = rs_bufs[g]
        half_copy(whole, whole, rs_send.at[g], rs_recv.at[g]).wait_send()
        half_copy(whole, whole, ag_send.at[g], ag_recv.at[g]).wait_send()


def ladder(mesh):
    devices = np.asarray(mesh.devices)
    axis = list(mesh.axis_names).index("ty")
    line = np.moveaxis(devices, axis, 0).reshape(devices.shape[axis], -1)[:, 0]
    coords = [getattr(d, "coords", None) for d in line]
    if len(line) != 8 or mesh.shape["tx"] != 2 or any(c is None for c in coords):
        return False
    steps = [[b - a for a, b in zip(coords[0], c)] for c in coords]
    rung, rail = steps[1], steps[2]
    unit = sum(abs(v) for v in rung) == 1 and sum(abs(v) for v in rail) == 1
    return unit and all(
        s == [k // 2 * v + k % 2 * w for v, w in zip(rail, rung)] for k, s in enumerate(steps))


def ladder_plan(n_fields, rows):
    chunks = [(f, 0, rows, "Q" if f % 3 == 2 else "P") for f in range(n_fields)]
    groups = [tuple(range(f, min(f + GROUP, n_fields))) for f in range(0, n_fields, GROUP)]
    return tuple(chunks), tuple(groups)


def ladder_kernel(
    n_ty, n_tx, chunks, groups,
    fields, weights_hbm, tile_s, block_s, coupling, driver_hbm, relaxation_hbm, row_tab, row_tab_t, col_tab,
    out, *scratch,
):
    n_fields, rows, cols = fields.shape
    n_chunks, n_groups = len(chunks), len(groups)
    gathered, asked, slots = (scratch[k * n_chunks : (k + 1) * n_chunks] for k in range(3))
    scratch = scratch[3 * n_chunks :]
    (modes, swapped, chip_sums, rs_bufs, sums, ag_bufs) = (
        scratch[k * n_groups : (k + 1) * n_groups] for k in range(6))
    (row_b, row_bt, col_b, weights, driver, relaxation, mine, rung_tile, rung_block, outer_tile, outer_block,
     tab_sem, own_sem, mine_sem, want_send, want_recv, sent, recv, mate_send, mate_recv,
     rs_send, rs_recv, ag_send, ag_recv, swap_send, swap_recv, back_send, back_recv) = scratch[6 * n_groups :]
    per_tile = cols // BS
    n_z = n_ty // 2
    n_ask = 2 * per_tile
    ty = lax.axis_index("ty")
    tx = lax.axis_index("tx")
    mate = 1 - tx
    z, y = ty // 2, ty % 2
    far_y = 1 - y
    left = z < n_z // 2
    end = (z == 0) | (z == n_z - 1)
    inner = jnp.logical_not(end)
    z_end = jnp.where(left, 0, n_z - 1)
    z_in = jnp.where(left, 1, n_z - 2)
    far_end, far_in = n_z - 1 - z_end, n_z - 1 - z_in
    rung = 2 * z + far_y
    across = 2 * far_in + y
    outer = 2 * z_end + y
    inward = 2 * z_in + y

    def copy_to(src, dst, send, got, where):
        return pltpu.make_async_remote_copy(
            src_ref=src, dst_ref=dst, send_sem=send, recv_sem=got, device_id=where, device_id_type=MESH)

    def tile(c, zz, yy, part=None, col=None):
        first, count = ((tx if col is None else col) * n_ty + yy * n_z + zz) * per_tile, per_tile
        if part is not None:
            count = per_tile // 2
            first = first + part * count
        return gathered[c].at[pl.ds(first, count)]

    def rail(c, col):
        return gathered[c].at[pl.ds((col * n_ty + y * n_z) * per_tile, n_z * per_tile)]

    def column(c, col):
        return gathered[c].at[pl.ds(col * n_ty * per_tile, n_ty * per_tile)]

    def send(c, ref, there, kind):
        copy_to(ref, ref, sent.at[c], recv.at[c, kind], {"ty": there}).start()

    def take(c, ref, kind):
        copy_to(ref, ref, sent.at[c], recv.at[c, kind], {"ty": rung}).wait_recv()

    def to_mate(c, ref):
        return copy_to(ref, ref, mate_send.at[c], mate_recv.at[c], {"tx": mate})

    E_OWN, E_FAR, I_ACROSS, E_ACROSS, I_PART, OWN_RUNG, E_RUNG, I_REST, ASKED = range(9)

    tabs = [
        pltpu.make_async_copy(row_tab.at[pl.ds(ty * rows, rows), :], row_b, tab_sem.at[0]),
        pltpu.make_async_copy(row_tab_t.at[:, pl.ds(pl.multiple_of(ty * rows, 128), rows)], row_bt, tab_sem.at[1]),
        pltpu.make_async_copy(col_tab.at[pl.ds(tx * cols, cols), :], col_b, tab_sem.at[2]),
        pltpu.make_async_copy(weights_hbm, weights, tab_sem.at[3]),
        pltpu.make_async_copy(driver_hbm, driver, tab_sem.at[4]),
        pltpu.make_async_copy(relaxation_hbm, relaxation, tab_sem.at[5]),
    ]

    barrier = pltpu.get_barrier_semaphore()
    pl.semaphore_signal(barrier, inc=1, device_id={"tx": mate}, device_id_type=MESH)
    for k in range(1, n_ty):
        pl.semaphore_signal(barrier, inc=1, device_id={"ty": (ty + k) % n_ty}, device_id_type=MESH)
    here = (tx * n_ty + y * n_z + z) * per_tile
    own = [
        [pltpu.make_async_copy(fields.at[f, pl.ds(r0, nr), pl.ds(b * BS, BS)], gathered[c].at[here + b], own_sem.at[c, b])
         for b in range(per_tile)]
        for c, (f, r0, nr, _) in enumerate(chunks)
    ]
    mine_copy = pltpu.make_async_copy(fields, mine, mine_sem)
    for copies in own:
        for copy in copies:
            copy.start()
    for copy in [mine_copy] + tabs:
        copy.start()
    pl.semaphore_wait(barrier, n_ty)

    want = [
        (copy_to(tile_s, rung_tile, want_send.at[0], want_recv.at[0], {"ty": rung}),
         copy_to(block_s, rung_block, want_send.at[1], want_recv.at[1], {"ty": rung})),
        (copy_to(tile_s, outer_tile, want_send.at[2], want_recv.at[2], {"ty": inward}),
         copy_to(block_s, outer_block, want_send.at[3], want_recv.at[3], {"ty": inward})),
    ]
    for copy in want[0]:
        copy.start()

    @pl.when(end)
    def _():
        for copy in want[1]:
            copy.start()

    def spot(tiles, blocks, s, j):
        t = tiles[s, j]
        row, col = lax.div(t, n_tx), lax.rem(t, n_tx)
        row_z, row_y = lax.div(row, 2), lax.rem(row, 2)
        return col, row_z, row_y, blocks[s, j]

    def place(col, row_z, row_y, block):
        return (col * n_ty + row_y * n_z + row_z) * per_tile + block

    def launch(c):
        for copy in own[c]:
            copy.wait()
        ref = tile(c, z, y)
        if chunks[c][3] == "P":
            @pl.when(inner)
            def _():
                send(c, ref, rung, OWN_RUNG)
                send(c, ref, across, I_ACROSS)
                to_mate(c, ref).start()

            @pl.when(end)
            def _():
                send(c, ref, rung, OWN_RUNG)
                send(c, ref, inward, E_OWN)
        else:
            @pl.when(inner)
            def _():
                send(c, ref, across, I_ACROSS)
                send(c, ref, outer, E_OWN)

            @pl.when(end)
            def _():
                send(c, ref, inward, E_OWN)
            to_mate(c, ref).start()

    def first_hop(c):
        if chunks[c][3] == "P":
            @pl.when(inner)
            def _():
                ref = tile(c, z_end, y)
                take(c, ref, E_OWN)
                send(c, ref, across, E_ACROSS)
                to_mate(c, ref).start()
                ref = tile(c, z, far_y)
                take(c, ref, OWN_RUNG)
                send(c, tile(c, z, far_y, 0), across, I_PART)
                to_mate(c, ref).start()
                ref = tile(c, far_in, y)
                take(c, ref, I_ACROSS)
                send(c, tile(c, far_in, y, 1), rung, I_REST)
                to_mate(c, ref).start()

            @pl.when(end)
            def _():
                ref = tile(c, z, far_y)
                take(c, ref, OWN_RUNG)
                send(c, ref, inward, E_FAR)
        else:
            @pl.when(inner)
            def _():
                ref = tile(c, z_end, y)
                take(c, ref, E_OWN)
                send(c, ref, across, E_ACROSS)
                to_mate(c, ref).start()
                ref = tile(c, far_in, y)
                take(c, ref, I_ACROSS)
                send(c, ref, outer, I_ACROSS)
                to_mate(c, ref).start()

            @pl.when(end)
            def _():
                ref = tile(c, z_in, y)
                take(c, ref, E_OWN)
                to_mate(c, ref).start()

    def second_hop(c):
        if chunks[c][3] == "P":
            @pl.when(inner)
            def _():
                ref = tile(c, far_end, y)
                take(c, ref, E_ACROSS)
                send(c, ref, rung, E_RUNG)
                to_mate(c, ref).start()
                ref = tile(c, z_end, far_y)
                take(c, ref, E_FAR)
                to_mate(c, ref).start()
        else:
            @pl.when(inner)
            def _():
                ref = tile(c, far_end, y)
                take(c, ref, E_ACROSS)
                send(c, ref, outer, E_ACROSS)
                to_mate(c, ref).start()

            @pl.when(end)
            def _():
                ref = tile(c, far_in, y)
                take(c, ref, I_ACROSS)
                to_mate(c, ref).start()

    def answer(c):
        if chunks[c][3] == "P":
            @pl.when(inner)
            def _():
                take(c, tile(c, far_in, far_y, 0), I_PART)
                take(c, tile(c, far_in, far_y, 1), I_REST)
                to_mate(c, tile(c, far_in, far_y)).start()
                ref = tile(c, far_end, far_y)
                take(c, ref, E_RUNG)
                to_mate(c, ref).start()
                to_mate(c, column(c, mate)).wait_recv()
                for s in range(2):
                    for j in range(per_tile):
                        col, row_z, row_y, block = spot(outer_tile, outer_block, s, j)
                        asked[c][s * per_tile + j] = gathered[c][place(col, row_z, row_y, block)]
                copy_to(asked[c], slots[c], sent.at[c], recv.at[c, ASKED], {"ty": outer}).start()
        else:
            @pl.when(end)
            def _():
                ref = tile(c, far_end, y)
                take(c, ref, E_ACROSS)
                to_mate(c, ref).start()
            to_mate(c, rail(c, mate)).wait_recv()
            for s in range(2):
                for j in range(per_tile):
                    col, row_z, row_y, block = spot(rung_tile, rung_block, s, j)
                    asked[c][s * per_tile + j] = gathered[c][place(col, row_z, y, block)]
            copy_to(asked[c], slots[c], sent.at[c], recv.at[c, ASKED], {"ty": rung}).start()

    def blend(c):
        f, r0, nr, mode = chunks[c]
        whole = copy_to(asked[c], slots[c], sent.at[c], recv.at[c, ASKED], {"ty": rung})
        if mode == "P":
            @pl.when(end)
            def _():
                whole.wait_recv()
        else:
            whole.wait_recv()

        def source(s, j):
            col, row_z, row_y, block = spot(tile_s, block_s, s, j)
            if mode == "P":
                here_too = inner
                at = place(col, row_z, row_y, block)
            else:
                here_too = row_y == y
                at = place(col, row_z, y, block)
            return jnp.where(here_too, gathered[c][at].astype(jnp.float32), slots[c][s * per_tile + j].astype(jnp.float32))

        for j in range(per_tile):
            span = slice(j * BS, (j + 1) * BS)
            w = weights[r0 : r0 + nr, span].astype(jnp.float32)
            out[f, r0 : r0 + nr, span] = out[f, r0 : r0 + nr, span] + (w * source(0, j) + (1.0 - w) * source(1, j))

    def tendency(f):
        for b in range(per_tile):
            span = slice(b * BS, (b + 1) * BS)
            total = coupling[f : f + 1, 0:1].astype(jnp.float32) * mine[0, :, span].astype(jnp.float32)
            for k in range(1, n_fields):
                total = total + coupling[f : f + 1, k : k + 1].astype(jnp.float32) * mine[k, :, span].astype(jnp.float32)
            out[f, :, span] = total

    def project(g, f):
        col_modes = jnp.zeros((rows, 128), jnp.float32)
        for start in range(0, cols, 2 * BS):
            span = slice(start, start + 2 * BS)
            col_modes += jnp.dot(out[f, :, span], col_b[span, :], precision=HI, preferred_element_type=jnp.float32)
        part = jnp.dot(row_bt[...], col_modes, precision=HI, preferred_element_type=jnp.float32)
        modes[g][pl.ds((f - groups[g][0]) * 128, 128), :] = part
        if f == groups[g][-1]:
            swap_copy(g).start()

    def sizes(g):
        half = len(groups[g]) * 128 // n_tx
        return half, half // n_ty

    def swap_copy(g):
        half, _ = sizes(g)
        src = modes[g].at[pl.ds(pl.multiple_of(mate * half, 8), half), :]
        return copy_to(src, swapped[g], swap_send.at[g], swap_recv.at[g], {"tx": mate})

    def back_copy(g):
        half, _ = sizes(g)
        ref = ag_bufs[g].at[pl.ds(pl.multiple_of(tx * half, 8), half), :]
        return copy_to(ref, ref, back_send.at[g], back_recv.at[g], {"tx": mate})

    def rs_copy(g, k):
        _, span_rows = sizes(g)
        there = (ty + k) % n_ty
        src = chip_sums[g].at[pl.ds(pl.multiple_of(there * span_rows, 8), span_rows), :]
        return copy_to(src, rs_bufs[g].at[k - 1], rs_send.at[g], rs_recv.at[g], {"ty": there})

    def ag_copy(g, k):
        half, span_rows = sizes(g)
        there = (ty + k) % n_ty
        dst = ag_bufs[g].at[pl.ds(pl.multiple_of(tx * half + ty * span_rows, 8), span_rows), :]
        return copy_to(sums[g], dst, ag_send.at[g], ag_recv.at[g], {"ty": there})

    def scatter(g):
        half, _ = sizes(g)
        swap_copy(g).wait_recv()
        chip_sums[g][...] = modes[g][pl.ds(pl.multiple_of(tx * half, 8), half), :] + swapped[g][...]
        for k in range(1, n_ty):
            rs_copy(g, k).start()

    def reduce(g):
        half, span_rows = sizes(g)
        whole = rs_bufs[g]
        copy_to(whole, whole, rs_send.at[g], rs_recv.at[g], {"tx": mate}).wait_recv()
        part = chip_sums[g][pl.ds(pl.multiple_of(ty * span_rows, 8), span_rows), :]
        total = part + jnp.sum(rs_bufs[g][...], axis=0)
        sums[g][...] = total
        for k in range(1, n_ty):
            ag_copy(g, k).start()
        ag_bufs[g][pl.ds(pl.multiple_of(tx * half + ty * span_rows, 8), span_rows), :] = total

    def hand_back(g):
        whole = rs_bufs[g]
        copy_to(whole, whole, ag_send.at[g], ag_recv.at[g], {"tx": mate}).wait_recv()
        back_copy(g).start()

    def nudge(g):
        half, _ = sizes(g)
        ref = ag_bufs[g].at[pl.ds(pl.multiple_of(mate * half, 8), half), :]
        copy_to(ref, ref, back_send.at[g], back_recv.at[g], {"tx": mate}).wait_recv()
        for f in groups[g]:
            coef = ag_bufs[g][pl.ds((f - groups[g][0]) * 128, 128), :]
            term = relaxation[f] * (driver[f] - coef)
            recon = jnp.dot(row_b[...], term, precision=HI, preferred_element_type=jnp.float32)
            for start in range(0, cols, 2 * BS):
                span = slice(start, start + 2 * BS)
                out[f, :, span] += lax.dot_general(
                    recon, col_b[span, :], (((1,), (1,)), ((), ())), precision=HI, preferred_element_type=jnp.float32)

    last_chunk = {f: c for c, (f, _, _, _) in enumerate(chunks)}
    group_of = {f: g for g, fs in enumerate(groups) for f in fs}
    todo = []

    def work(count=1):
        for _ in range(min(count, len(todo))):
            step, g = todo.pop(0)
            step(g)

    def finish(c):
        blend(c)
        f = chunks[c][0]
        if last_chunk[f] == c:
            g = group_of[f]
            project(g, f)
            if f == groups[g][-1]:
                todo.extend([(scatter, g), (reduce, g), (hand_back, g), (nudge, g)])

    launch(0)
    mine_copy.wait()
    fresh = list(range(n_fields))
    launch(1)
    tendency(fresh.pop(0))
    for k in range(n_chunks + 2):
        if 0 < k and k + 1 < n_chunks:
            launch(k + 1)
        if k < n_chunks:
            first_hop(k)
        if fresh:
            tendency(fresh.pop(0))
        if k == 1:
            for copy in tabs:
                copy.wait()
            for copy in want[0]:
                copy.wait_recv()

            @pl.when(inner)
            def _():
                for copy in want[1]:
                    copy.wait_recv()
        if 0 <= k - 2:
            work(1)
            finish(k - 2)
        if 0 <= k - 1 < n_chunks:
            answer(k - 1)
            work(1)
        if k < n_chunks:
            second_hop(k)
    while todo:
        work(1)

    for c in range(n_chunks):
        mode = chunks[c][3]

        @pl.when(inner)
        def _():
            ref = gathered[c].at[pl.ds(0, 7 * per_tile)]
            copy_to(ref, ref, sent.at[c], recv.at[c, 0], {"ty": rung}).wait_send()
            if mode == "P":
                to_mate(c, column(c, tx)).wait_send()

        @pl.when(end)
        def _():
            ref = gathered[c].at[pl.ds(0, 3 * per_tile)]
            copy_to(ref, ref, sent.at[c], recv.at[c, 0], {"ty": rung}).wait_send()

        if mode == "Q":
            to_mate(c, rail(c, tx)).wait_send()
    for copy in want[0]:
        copy.wait_send()

    @pl.when(end)
    def _():
        for copy in want[1]:
            copy.wait_send()
    for g in range(n_groups):
        swap_copy(g).wait_send()
        back_copy(g).wait_send()
        whole = rs_bufs[g]
        copy_to(whole, whole, rs_send.at[g], rs_recv.at[g], {"tx": mate}).wait_send()
        copy_to(whole, whole, ag_send.at[g], ag_recv.at[g], {"tx": mate}).wait_send()


def ladder_call(
    n_ty, n_tx, fields, weights, tile, block, coupling, driver, relaxation, row_tab, row_tab_t, col_tab,
):
    n_fields, rows, cols = fields.shape
    chunks, groups = ladder_plan(n_fields, rows)
    n_chunks, n_groups = len(chunks), len(groups)
    per_tile = cols // BS
    vmem = pl.BlockSpec(memory_space=pltpu.VMEM)
    smem = pl.BlockSpec(memory_space=pltpu.SMEM)
    hbm = pl.BlockSpec(memory_space=pltpu.HBM)
    dma = pltpu.SemaphoreType.DMA
    halves = [len(g) * 128 // n_tx for g in groups]
    asks = pltpu.SMEM((2, per_tile), jnp.int32)
    scratch = (
        [pltpu.VMEM((n_ty * n_tx * per_tile, c[2], BS), jnp.bfloat16) for c in chunks]
        + [pltpu.VMEM((2 * per_tile, c[2], BS), jnp.bfloat16) for c in chunks] * 2
        + [pltpu.VMEM((len(g) * 128, 128), jnp.float32) for g in groups]
        + [pltpu.VMEM((h, 128), jnp.float32) for h in halves] * 2
        + [pltpu.VMEM((n_ty - 1, h // n_ty, 128), jnp.float32) for h in halves]
        + [pltpu.VMEM((h // n_ty, 128), jnp.float32) for h in halves]
        + [pltpu.VMEM((len(g) * 128, 128), jnp.float32) for g in groups]
        + [
            pltpu.VMEM((rows, 128), jnp.float32),
            pltpu.VMEM((128, rows), jnp.float32),
            pltpu.VMEM((cols, 128), jnp.float32),
            pltpu.VMEM((rows, cols), jnp.bfloat16),
            pltpu.VMEM(driver.shape, jnp.float32),
            pltpu.VMEM(relaxation.shape, jnp.float32),
            pltpu.VMEM(fields.shape, jnp.bfloat16),
            asks, asks, asks, asks,
            dma((6,)),
            dma((n_chunks, per_tile)),
            dma,
            dma((4,)),
            dma((4,)),
            dma((n_chunks,)),
            dma((n_chunks, 9)),
            dma((n_chunks,)),
            dma((n_chunks,)),
            *[dma((n_groups,))] * 8,
        ]
    )
    return pl.pallas_call(
        functools.partial(ladder_kernel, n_ty, n_tx, chunks, groups),
        out_shape=jax.ShapeDtypeStruct((n_fields, rows, cols), jnp.float32),
        in_specs=[hbm, hbm, smem, smem, vmem, hbm, hbm, hbm, hbm, hbm],
        out_specs=vmem,
        scratch_shapes=scratch,
        compiler_params=pltpu.CompilerParams(
            collective_id=0, has_side_effects=True, vmem_limit_bytes=67043328
        ),
        name="remap_ladder",
    )(fields, weights, tile, block, coupling, driver, relaxation, row_tab, row_tab_t, col_tab)


def solution(mesh):
    n_ty, n_tx = mesh.shape["ty"], mesh.shape["tx"]
    snake = two_lines(mesh)
    rungs = ladder(mesh)

    def body(fields, weights, source_tile, source_block, coupling, driver, relaxation):
        n_fields, rows, cols = fields.shape
        n_groups = n_fields // GROUP
        n_dev = n_ty * n_tx
        half = GROUP * 128 // n_tx
        span_rows = half // n_ty
        row_np, col_np = wave_table(rows * n_ty), wave_table(cols * n_tx)
        row_tab, row_tab_t = jnp.asarray(row_np), jnp.asarray(np.ascontiguousarray(row_np.T))
        if row_np.shape == col_np.shape:
            col_tab = row_tab
        else:
            col_tab = jnp.asarray(col_np)
        tile = jnp.transpose(source_tile, (0, 2, 1))[0]
        block = jnp.transpose(source_block, (0, 2, 1))[0]
        if rungs:
            return ladder_call(
                n_ty, n_tx, fields, weights, tile, block, coupling, driver, relaxation, row_tab, row_tab_t, col_tab)
        picks = (tile % n_tx * n_ty + tile // n_tx) * (cols // BS) + block
        vmem = pl.BlockSpec(memory_space=pltpu.VMEM)
        smem = pl.BlockSpec(memory_space=pltpu.SMEM)
        hbm = pl.BlockSpec(memory_space=pltpu.HBM)
        dma = pltpu.SemaphoreType.DMA
        scratch = (
            [pltpu.VMEM((n_dev * (cols // BS), BS, BS), jnp.bfloat16)] * n_fields
            + [pltpu.VMEM((GROUP * 128, 128), jnp.float32)] * n_groups
            + [pltpu.VMEM((half, 128), jnp.float32)] * (2 * n_groups)
            + [pltpu.VMEM((n_ty - 1, span_rows, 128), jnp.float32)] * n_groups
            + [pltpu.VMEM((span_rows, 128), jnp.float32)] * n_groups
            + [pltpu.VMEM((GROUP * 128, 128), jnp.float32)] * n_groups
            + [
                pltpu.VMEM((rows, 128), jnp.float32),
                pltpu.VMEM((128, rows), jnp.float32),
                pltpu.VMEM((cols, 128), jnp.float32),
                pltpu.VMEM((rows, cols), jnp.bfloat16),
                pltpu.VMEM(driver.shape, jnp.float32),
                pltpu.VMEM(relaxation.shape, jnp.float32),
                dma((6,)),
                dma((n_fields, cols // BS)),
                dma((n_fields,)),
                dma((n_fields, 2, 2, n_ty // 2)),
                dma((n_fields,)),
                dma((n_fields,)),
                *[dma((n_groups,))] * 8,
            ]
        )
        return pl.pallas_call(
            functools.partial(ring_kernel, n_ty, n_tx, snake),
            out_shape=jax.ShapeDtypeStruct((n_fields, rows, cols), jnp.float32),
            in_specs=[hbm, hbm, smem, vmem, hbm, hbm, hbm, hbm, hbm],
            out_specs=vmem,
            scratch_shapes=scratch,
            compiler_params=pltpu.CompilerParams(
                collective_id=0, has_side_effects=True, vmem_limit_bytes=67043328
            ),
            name="remap_nudge",
        )(fields, weights, picks, coupling, driver, relaxation, row_tab, row_tab_t, col_tab)

    in_specs = (
        P(None, ("groups", "ty"), "tx"),
        P(("groups", "ty"), "tx"),
        P(("groups", "ty"), "tx", None),
        P(("groups", "ty"), "tx", None),
        P(),
        P(),
        P(),
    )
    out_specs = P(None, ("groups", "ty"), "tx")
    return jax.shard_map(body, mesh=mesh, in_specs=in_specs, out_specs=out_specs, check_vma=False)
```

```python
import functools
import math

import jax
import jax.numpy as jnp
import numpy as np
from jax import lax
from jax.experimental import pallas as pl
from jax.experimental.pallas import tpu as pltpu
from jax.sharding import PartitionSpec as P

BS = 128
KMAX = 64
GROUP = 2
MESH = pl.DeviceIdType.MESH
HI = lax.Precision.HIGHEST


def wave_table(period):
    position = np.arange(period, dtype=np.int64)[:, None]
    mode = np.arange(KMAX, dtype=np.int64)[None, :]
    norming = np.where(mode == 0, math.sqrt(1.0 / period), math.sqrt(2.0 / period))
    cos_part = np.cos(2.0 * math.pi * (position * mode % period) / period) * norming
    sin_part = np.sin(2.0 * math.pi * (position * (mode + 1) % period) / period) * math.sqrt(2.0 / period)
    return np.concatenate([cos_part, sin_part], axis=1).astype(np.float32)


def two_lines(mesh):
    devices = np.asarray(mesh.devices)
    axis = list(mesh.axis_names).index("ty")
    line = np.moveaxis(devices, axis, 0).reshape(devices.shape[axis], -1)[:, 0]
    coords = [getattr(d, "coords", None) for d in line]
    if any(c is None for c in coords) or len(line) % 2:
        return False
    varying = [k for k in range(len(coords[0])) if len({c[k] for c in coords}) > 1]
    return len(varying) > 1


def ring_kernel(
    n_ty, n_tx, snake,
    fields, weights_hbm, picks, coupling, driver_hbm, relaxation_hbm, row_tab, row_tab_t, col_tab,
    out, *scratch,
):
    n_fields, rows, cols = fields.shape
    gathered = scratch[:n_fields]
    n_groups = n_fields // GROUP
    (modes, swapped, chip_sums, rs_bufs, sums, ag_bufs) = (
        scratch[n_fields + k * n_groups : n_fields + (k + 1) * n_groups] for k in range(6))
    (row_b, row_bt, col_b, weights, driver, relaxation, tab_sem, own_sem, ring_send, ring_recv, mate_send, mate_recv,
     rs_send, rs_recv, ag_send, ag_recv, swap_send, swap_recv, back_send, back_recv) = scratch[n_fields + 6 * n_groups :]
    per_tile = cols // BS
    ty = lax.axis_index("ty")
    tx = lax.axis_index("tx")
    mate = 1 - tx
    depth = n_ty // 2

    def ring_to_ty(pos):
        pos = (pos + n_ty) % n_ty
        if not snake:
            return pos
        return jnp.where(pos < n_ty // 2, 2 * pos, 2 * (n_ty - 1 - pos) + 1)

    ring = jnp.where(ty % 2 == 0, ty // 2, n_ty - 1 - ty // 2) if snake else ty
    toward = (ring_to_ty(ring + 1), ring_to_ty(ring - 1))

    tabs = [
        pltpu.make_async_copy(row_tab.at[pl.ds(ty * rows, rows), :], row_b, tab_sem.at[0]),
        pltpu.make_async_copy(row_tab_t.at[:, pl.ds(pl.multiple_of(ty * rows, 128), rows)], row_bt, tab_sem.at[1]),
        pltpu.make_async_copy(col_tab.at[pl.ds(tx * cols, cols), :], col_b, tab_sem.at[2]),
        pltpu.make_async_copy(weights_hbm, weights, tab_sem.at[3]),
        pltpu.make_async_copy(driver_hbm, driver, tab_sem.at[4]),
        pltpu.make_async_copy(relaxation_hbm, relaxation, tab_sem.at[5]),
    ]

    def tile_of(f, col, row, part=None):
        first, count = (col * n_ty + row) * per_tile, per_tile
        if part is not None:
            count = per_tile // 2
            first = first + part * count
        return gathered[f].at[pl.ds(first, count)]

    def column_of(f, col):
        return gathered[f].at[pl.ds(col * n_ty * per_tile, n_ty * per_tile)]

    barrier = pltpu.get_barrier_semaphore()
    pl.semaphore_signal(barrier, inc=1, device_id={"tx": mate}, device_id_type=MESH)
    for k in range(1, n_ty):
        pl.semaphore_signal(barrier, inc=1, device_id={"ty": (ty + k) % n_ty}, device_id_type=MESH)
    here = (tx * n_ty + ty) * per_tile

    own = [
        pltpu.make_async_copy(fields.at[f, :, pl.ds(b * BS, BS)], gathered[f].at[here + b], own_sem.at[f, b])
        for f in range(n_fields)
        for b in range(per_tile)
    ]
    for copy in own + tabs:
        copy.start()
    pl.semaphore_wait(barrier, n_ty)
    for copy in own:
        copy.wait()

    def to_mate(f, ref):
        return pltpu.make_async_remote_copy(
            src_ref=ref, dst_ref=ref, send_sem=mate_send.at[f], recv_sem=mate_recv.at[f],
            device_id={"tx": mate}, device_id_type=MESH)

    def sign(way):
        return 1 if way == 0 else -1

    def travels(way, h, d):
        return d < depth - 1 or (d == depth - 1 and h == way)

    def ring_copy(f, way, h, d):
        ref = tile_of(f, tx, ring_to_ty(ring - sign(way) * d), h)
        return pltpu.make_async_remote_copy(
            src_ref=ref, dst_ref=ref,
            send_sem=ring_send.at[f], recv_sem=ring_recv.at[f, way, h, d],
            device_id={"ty": toward[way]}, device_id_type=MESH)

    def arrived(f, way, h, d):
        ref = tile_of(f, tx, ring_to_ty(ring - sign(way) * (d + 1)), h)
        pltpu.make_async_remote_copy(
            src_ref=ref, dst_ref=ref, send_sem=ring_send.at[f], recv_sem=ring_recv.at[f, way, h, d],
            device_id={"ty": toward[way]}, device_id_type=MESH).wait_recv()
        return ref

    def stage(g, d):
        for f in range(g * GROUP, (g + 1) * GROUP):
            for h in range(2):
                for way in range(2):
                    came = d > 0 and travels(way, h, d - 1)
                    if came:
                        got = arrived(f, way, h, d - 1)
                    if travels(way, h, d):
                        ring_copy(f, way, h, d).start()
                    if came:
                        to_mate(f, got).start()
            if d == 0:
                to_mate(f, tile_of(f, tx, ty)).start()

    def tendency(g):
        for f in range(g * GROUP, (g + 1) * GROUP):
            for b in range(per_tile):
                span = slice(b * BS, (b + 1) * BS)
                total = coupling[f : f + 1, 0:1].astype(jnp.float32) * gathered[0][here + b].astype(jnp.float32)
                for k in range(1, n_fields):
                    total = total + coupling[f : f + 1, k : k + 1].astype(jnp.float32) * gathered[k][here + b].astype(jnp.float32)
                out[f, :, span] = total

    def upstream(g):
        for f in range(g * GROUP, (g + 1) * GROUP):
            to_mate(f, column_of(f, mate)).wait_recv()
            for j in range(per_tile):
                span = slice(j * BS, (j + 1) * BS)

                first = gathered[f][picks[0, j]].astype(jnp.float32)
                second = gathered[f][picks[1, j]].astype(jnp.float32)
                w = weights[:, span].astype(jnp.float32)
                out[f, :, span] = out[f, :, span] + (w * first + (1.0 - w) * second)
            col_modes = jnp.zeros((rows, 128), jnp.float32)
            for start in range(0, cols, 2 * BS):
                span = slice(start, start + 2 * BS)
                col_modes += jnp.dot(out[f, :, span], col_b[span, :], precision=HI, preferred_element_type=jnp.float32)
            part = jnp.dot(row_bt[...], col_modes, precision=HI, preferred_element_type=jnp.float32)
            modes[g][pl.ds((f - g * GROUP) * 128, 128), :] = part
        swap_copy(g).start()

    half = GROUP * 128 // n_tx
    span_rows = half // n_ty

    def half_copy(src, dst, send, recv):
        return pltpu.make_async_remote_copy(
            src_ref=src, dst_ref=dst, send_sem=send, recv_sem=recv, device_id={"tx": mate}, device_id_type=MESH)

    def swap_copy(g):
        src = modes[g].at[pl.ds(pl.multiple_of(mate * half, 8), half), :]
        return half_copy(src, swapped[g], swap_send.at[g], swap_recv.at[g])

    def back_copy(g):
        ref = ag_bufs[g].at[pl.ds(pl.multiple_of(tx * half, 8), half), :]
        return half_copy(ref, ref, back_send.at[g], back_recv.at[g])

    def rs_copy(g, k):
        there = (ty + k) % n_ty
        return pltpu.make_async_remote_copy(
            src_ref=chip_sums[g].at[pl.ds(pl.multiple_of(there * span_rows, 8), span_rows), :], dst_ref=rs_bufs[g].at[k - 1],
            send_sem=rs_send.at[g], recv_sem=rs_recv.at[g], device_id={"ty": there}, device_id_type=MESH)

    def ag_copy(g, k):
        there = (ty + k) % n_ty
        return pltpu.make_async_remote_copy(
            src_ref=sums[g], dst_ref=ag_bufs[g].at[pl.ds(pl.multiple_of(tx * half + ty * span_rows, 8), span_rows), :],
            send_sem=ag_send.at[g], recv_sem=ag_recv.at[g], device_id={"ty": there}, device_id_type=MESH)

    def scatter(g):
        swap_copy(g).wait_recv()
        chip_sums[g][...] = modes[g][pl.ds(pl.multiple_of(tx * half, 8), half), :] + swapped[g][...]
        for k in range(1, n_ty):
            rs_copy(g, k).start()

    def reduce(g):
        whole = rs_bufs[g]
        half_copy(whole, whole, rs_send.at[g], rs_recv.at[g]).wait_recv()
        mine = chip_sums[g][pl.ds(pl.multiple_of(ty * span_rows, 8), span_rows), :]
        total = mine + jnp.sum(rs_bufs[g][...], axis=0)
        sums[g][...] = total
        for k in range(1, n_ty):
            ag_copy(g, k).start()
        ag_bufs[g][pl.ds(pl.multiple_of(tx * half + ty * span_rows, 8), span_rows), :] = total

    def hand_back(g):
        whole = rs_bufs[g]
        half_copy(whole, whole, ag_send.at[g], ag_recv.at[g]).wait_recv()
        back_copy(g).start()

    def nudge(g):
        ref = ag_bufs[g].at[pl.ds(pl.multiple_of(mate * half, 8), half), :]
        half_copy(ref, ref, back_send.at[g], back_recv.at[g]).wait_recv()
        for f in range(g * GROUP, (g + 1) * GROUP):
            coef = ag_bufs[g][pl.ds((f - g * GROUP) * 128, 128), :]
            term = relaxation[f] * (driver[f] - coef)
            recon = jnp.dot(row_b[...], term, precision=HI, preferred_element_type=jnp.float32)
            for start in range(0, cols, 2 * BS):
                span = slice(start, start + 2 * BS)
                out[f, :, span] += lax.dot_general(
                    recon, col_b[span, :], (((1,), (1,)), ((), ())), precision=HI, preferred_element_type=jnp.float32)

    stage(0, 0)
    for g in range(n_groups):
        tendency(g)
    for copy in tabs:
        copy.wait()
    end = n_groups - 1
    for g in range(end):
        behind = [upstream, scatter, reduce] if g > 0 else []
        for d in range(1, depth):
            stage(g, d)
            if behind:
                behind.pop(0)(g - 1)
        stage(g + 1, 0)
        stage(g, depth)
        if g > 0:
            for step in behind + [hand_back, nudge]:
                step(g - 1)
    for d in range(1, depth):
        stage(end, d)
        if d == 1:
            upstream(end - 1)
    scatter(end - 1)
    stage(end, depth)
    reduce(end - 1)
    upstream(end)
    scatter(end)
    hand_back(end - 1)
    reduce(end)
    nudge(end - 1)
    hand_back(end)
    nudge(end)

    for f in range(n_fields):
        sent = gathered[f].at[pl.ds(0, (n_ty - 1) * per_tile)]
        pltpu.make_async_remote_copy(
            src_ref=sent, dst_ref=sent, send_sem=ring_send.at[f], recv_sem=ring_recv.at[f, 0, 0, 0],
            device_id={"ty": toward[0]}, device_id_type=MESH).wait_send()
        to_mate(f, column_of(f, tx)).wait_send()
    for g in range(n_groups):
        swap_copy(g).wait_send()
        back_copy(g).wait_send()
        whole = rs_bufs[g]
        half_copy(whole, whole, rs_send.at[g], rs_recv.at[g]).wait_send()
        half_copy(whole, whole, ag_send.at[g], ag_recv.at[g]).wait_send()


def ladder(mesh):
    devices = np.asarray(mesh.devices)
    axis = list(mesh.axis_names).index("ty")
    line = np.moveaxis(devices, axis, 0).reshape(devices.shape[axis], -1)[:, 0]
    coords = [getattr(d, "coords", None) for d in line]
    if len(line) != 8 or mesh.shape["tx"] != 2 or any(c is None for c in coords):
        return False
    steps = [[b - a for a, b in zip(coords[0], c)] for c in coords]
    rung, rail = steps[1], steps[2]
    unit = sum(abs(v) for v in rung) == 1 and sum(abs(v) for v in rail) == 1
    return unit and all(
        s == [k // 2 * v + k % 2 * w for v, w in zip(rail, rung)] for k, s in enumerate(steps))


SPLIT = 2
PATTERN = "QPP"
LAUNCH, SECOND, COLLECT, ANSWER, FINISH = 3, 1, 2, 3, 5
ADDS = (1, 2, 2, 2)


def ladder_plan(n_fields, rows):
    pieces = SPLIT if rows % (16 * SPLIT) == 0 else 1
    size = rows // pieces
    spots = [(f, r) for f in range(n_fields) for r in range(0, rows, size)]
    chunks = [(f, r, size, PATTERN[k % len(PATTERN)]) for k, (f, r) in enumerate(spots)]
    groups = [tuple(range(f, min(f + GROUP, n_fields))) for f in range(0, n_fields, GROUP)]
    return tuple(chunks), tuple(groups)


def ladder_kernel(
    n_ty, n_tx, chunks, groups,
    fields, weights_hbm, tile_s, block_s, coupling, driver_hbm, relaxation_hbm, row_tab, row_tab_t, col_tab,
    out, *scratch,
):
    n_fields, rows, cols = fields.shape
    n_chunks, n_groups = len(chunks), len(groups)
    gathered, asked, slots = (scratch[k * n_chunks : (k + 1) * n_chunks] for k in range(3))
    scratch = scratch[3 * n_chunks :]
    (modes, swapped, chip_sums, rs_bufs, sums, ag_bufs) = (
        scratch[k * n_groups : (k + 1) * n_groups] for k in range(6))
    (row_b, row_bt, col_b, weights, driver, relaxation, mine, rung_tile, rung_block, outer_tile, outer_block,
     tab_sem, own_sem, mine_sem, want_send, want_recv, sent, recv, mate_send, mate_recv,
     rs_send, rs_recv, ag_send, ag_recv, swap_send, swap_recv, back_send, back_recv) = scratch[6 * n_groups :]
    per_tile = cols // BS
    n_z = n_ty // 2
    n_ask = 2 * per_tile
    ty = lax.axis_index("ty")
    tx = lax.axis_index("tx")
    mate = 1 - tx
    z, y = ty // 2, ty % 2
    far_y = 1 - y
    left = z < n_z // 2
    end = (z == 0) | (z == n_z - 1)
    inner = jnp.logical_not(end)
    z_end = jnp.where(left, 0, n_z - 1)
    z_in = jnp.where(left, 1, n_z - 2)
    far_end, far_in = n_z - 1 - z_end, n_z - 1 - z_in
    rung = 2 * z + far_y
    across = 2 * far_in + y
    outer = 2 * z_end + y
    inward = 2 * z_in + y

    def copy_to(src, dst, send, got, where):
        return pltpu.make_async_remote_copy(
            src_ref=src, dst_ref=dst, send_sem=send, recv_sem=got, device_id=where, device_id_type=MESH)

    def tile(c, zz, yy, part=None, col=None):
        first, count = ((tx if col is None else col) * n_ty + yy * n_z + zz) * per_tile, per_tile
        if part is not None:
            count = per_tile // 2
            first = first + part * count
        return gathered[c].at[pl.ds(first, count)]

    def rail(c, col):
        return gathered[c].at[pl.ds((col * n_ty + y * n_z) * per_tile, n_z * per_tile)]

    def column(c, col):
        return gathered[c].at[pl.ds(col * n_ty * per_tile, n_ty * per_tile)]

    def send(c, ref, there, kind):
        copy_to(ref, ref, sent.at[c], recv.at[c, kind], {"ty": there}).start()

    def take(c, ref, kind):
        copy_to(ref, ref, sent.at[c], recv.at[c, kind], {"ty": rung}).wait_recv()

    def to_mate(c, ref):
        return copy_to(ref, ref, mate_send.at[c], mate_recv.at[c], {"tx": mate})

    E_OWN, E_FAR, I_ACROSS, E_ACROSS, I_PART, OWN_RUNG, E_RUNG, I_REST, ASKED = range(9)

    tabs = [
        pltpu.make_async_copy(row_tab.at[pl.ds(ty * rows, rows), :], row_b, tab_sem.at[0]),
        pltpu.make_async_copy(row_tab_t.at[:, pl.ds(pl.multiple_of(ty * rows, 128), rows)], row_bt, tab_sem.at[1]),
        pltpu.make_async_copy(col_tab.at[pl.ds(tx * cols, cols), :], col_b, tab_sem.at[2]),
        pltpu.make_async_copy(weights_hbm, weights, tab_sem.at[3]),
        pltpu.make_async_copy(driver_hbm, driver, tab_sem.at[4]),
        pltpu.make_async_copy(relaxation_hbm, relaxation, tab_sem.at[5]),
    ]

    barrier = pltpu.get_barrier_semaphore()
    pl.semaphore_signal(barrier, inc=1, device_id={"tx": mate}, device_id_type=MESH)
    for k in range(1, n_ty):
        pl.semaphore_signal(barrier, inc=1, device_id={"ty": (ty + k) % n_ty}, device_id_type=MESH)
    here = (tx * n_ty + y * n_z + z) * per_tile
    own = [
        [pltpu.make_async_copy(fields.at[f, pl.ds(r0, nr), pl.ds(b * BS, BS)], gathered[c].at[here + b], own_sem.at[c, b])
         for b in range(per_tile)]
        for c, (f, r0, nr, _) in enumerate(chunks)
    ]
    mine_copy = pltpu.make_async_copy(fields, mine, mine_sem)
    for copies in own:
        for copy in copies:
            copy.start()
    for copy in [mine_copy] + tabs:
        copy.start()
    pl.semaphore_wait(barrier, n_ty)

    want = [
        (copy_to(tile_s, rung_tile, want_send.at[0], want_recv.at[0], {"ty": rung}),
         copy_to(block_s, rung_block, want_send.at[1], want_recv.at[1], {"ty": rung})),
        (copy_to(tile_s, outer_tile, want_send.at[2], want_recv.at[2], {"ty": inward}),
         copy_to(block_s, outer_block, want_send.at[3], want_recv.at[3], {"ty": inward})),
    ]
    for copy in want[0]:
        copy.start()

    @pl.when(end)
    def _():
        for copy in want[1]:
            copy.start()

    def spot(tiles, blocks, s, j):
        t = tiles[s, j]
        row, col = lax.div(t, n_tx), lax.rem(t, n_tx)
        row_z, row_y = lax.div(row, 2), lax.rem(row, 2)
        return col, row_z, row_y, blocks[s, j]

    def place(col, row_z, row_y, block):
        return (col * n_ty + row_y * n_z + row_z) * per_tile + block

    def launch(c):
        for copy in own[c]:
            copy.wait()
        ref = tile(c, z, y)
        if chunks[c][3] == "P":
            @pl.when(inner)
            def _():
                send(c, ref, rung, OWN_RUNG)
                send(c, ref, across, I_ACROSS)
                to_mate(c, ref).start()

            @pl.when(end)
            def _():
                send(c, ref, rung, OWN_RUNG)
                send(c, ref, inward, E_OWN)
        else:
            @pl.when(inner)
            def _():
                send(c, ref, across, I_ACROSS)
                send(c, ref, outer, E_OWN)

            @pl.when(end)
            def _():
                send(c, ref, inward, E_OWN)
            to_mate(c, ref).start()

    def first_hop(c):
        if chunks[c][3] == "P":
            @pl.when(inner)
            def _():
                ref = tile(c, z_end, y)
                take(c, ref, E_OWN)
                send(c, ref, across, E_ACROSS)
                to_mate(c, ref).start()
                ref = tile(c, z, far_y)
                take(c, ref, OWN_RUNG)
                send(c, tile(c, z, far_y, 0), across, I_PART)
                to_mate(c, ref).start()
                ref = tile(c, far_in, y)
                take(c, ref, I_ACROSS)
                send(c, tile(c, far_in, y, 1), rung, I_REST)
                to_mate(c, ref).start()

            @pl.when(end)
            def _():
                ref = tile(c, z, far_y)
                take(c, ref, OWN_RUNG)
                send(c, ref, inward, E_FAR)
        else:
            @pl.when(inner)
            def _():
                ref = tile(c, z_end, y)
                take(c, ref, E_OWN)
                send(c, ref, across, E_ACROSS)
                to_mate(c, ref).start()
                ref = tile(c, far_in, y)
                take(c, ref, I_ACROSS)
                send(c, ref, outer, I_ACROSS)
                to_mate(c, ref).start()

            @pl.when(end)
            def _():
                ref = tile(c, z_in, y)
                take(c, ref, E_OWN)
                to_mate(c, ref).start()

    def second_hop(c):
        if chunks[c][3] == "P":
            @pl.when(inner)
            def _():
                ref = tile(c, far_end, y)
                take(c, ref, E_ACROSS)
                send(c, ref, rung, E_RUNG)
                to_mate(c, ref).start()
                ref = tile(c, z_end, far_y)
                take(c, ref, E_FAR)
                to_mate(c, ref).start()
        else:
            @pl.when(inner)
            def _():
                ref = tile(c, far_end, y)
                take(c, ref, E_ACROSS)
                send(c, ref, outer, E_ACROSS)
                to_mate(c, ref).start()

            @pl.when(end)
            def _():
                ref = tile(c, far_in, y)
                take(c, ref, I_ACROSS)
                to_mate(c, ref).start()

    def collect(c):
        if chunks[c][3] == "P":
            @pl.when(inner)
            def _():
                take(c, tile(c, far_in, far_y, 0), I_PART)
                take(c, tile(c, far_in, far_y, 1), I_REST)
                to_mate(c, tile(c, far_in, far_y)).start()
                ref = tile(c, far_end, far_y)
                take(c, ref, E_RUNG)
                to_mate(c, ref).start()
        else:
            @pl.when(end)
            def _():
                ref = tile(c, far_end, y)
                take(c, ref, E_ACROSS)
                to_mate(c, ref).start()

    def answer(c):
        if chunks[c][3] == "P":
            @pl.when(inner)
            def _():
                to_mate(c, column(c, mate)).wait_recv()
                for s in range(2):
                    for j in range(per_tile):
                        col, row_z, row_y, block = spot(outer_tile, outer_block, s, j)
                        asked[c][s * per_tile + j] = gathered[c][place(col, row_z, row_y, block)]
                copy_to(asked[c], slots[c], sent.at[c], recv.at[c, ASKED], {"ty": outer}).start()
        else:
            to_mate(c, rail(c, mate)).wait_recv()
            for s in range(2):
                for j in range(per_tile):
                    col, row_z, row_y, block = spot(rung_tile, rung_block, s, j)
                    asked[c][s * per_tile + j] = gathered[c][place(col, row_z, y, block)]
            copy_to(asked[c], slots[c], sent.at[c], recv.at[c, ASKED], {"ty": rung}).start()

    def blend(c):
        f, r0, nr, mode = chunks[c]
        whole = copy_to(asked[c], slots[c], sent.at[c], recv.at[c, ASKED], {"ty": rung})
        if mode == "P":
            @pl.when(end)
            def _():
                whole.wait_recv()
        else:
            whole.wait_recv()

        def source(s, j):
            col, row_z, row_y, block = spot(tile_s, block_s, s, j)
            if mode == "P":
                here_too = inner
                at = place(col, row_z, row_y, block)
            else:
                here_too = row_y == y
                at = place(col, row_z, y, block)
            return jnp.where(here_too, gathered[c][at].astype(jnp.float32), slots[c][s * per_tile + j].astype(jnp.float32))

        for j in range(per_tile):
            span = slice(j * BS, (j + 1) * BS)
            w = weights[r0 : r0 + nr, span].astype(jnp.float32)
            out[f, r0 : r0 + nr, span] = out[f, r0 : r0 + nr, span] + (w * source(0, j) + (1.0 - w) * source(1, j))

    def tendency(f):
        for b in range(per_tile):
            span = slice(b * BS, (b + 1) * BS)
            total = coupling[f : f + 1, 0:1].astype(jnp.float32) * mine[0, :, span].astype(jnp.float32)
            for k in range(1, n_fields):
                total = total + coupling[f : f + 1, k : k + 1].astype(jnp.float32) * mine[k, :, span].astype(jnp.float32)
            out[f, :, span] = total

    def project(g, f):
        col_modes = jnp.zeros((rows, 128), jnp.float32)
        for start in range(0, cols, 2 * BS):
            span = slice(start, start + 2 * BS)
            col_modes += jnp.dot(out[f, :, span], col_b[span, :], precision=HI, preferred_element_type=jnp.float32)
        part = jnp.dot(row_bt[...], col_modes, precision=HI, preferred_element_type=jnp.float32)
        modes[g][pl.ds((f - groups[g][0]) * 128, 128), :] = part
        if f == groups[g][-1]:
            swap_copy(g).start()

    def sizes(g):
        half = len(groups[g]) * 128 // n_tx
        return half, half // n_ty

    def swap_copy(g):
        half, _ = sizes(g)
        src = modes[g].at[pl.ds(pl.multiple_of(mate * half, 8), half), :]
        return copy_to(src, swapped[g], swap_send.at[g], swap_recv.at[g], {"tx": mate})

    def back_copy(g):
        half, _ = sizes(g)
        ref = ag_bufs[g].at[pl.ds(pl.multiple_of(tx * half, 8), half), :]
        return copy_to(ref, ref, back_send.at[g], back_recv.at[g], {"tx": mate})

    def rs_copy(g, k):
        _, span_rows = sizes(g)
        there = (ty + k) % n_ty
        src = chip_sums[g].at[pl.ds(pl.multiple_of(there * span_rows, 8), span_rows), :]
        return copy_to(src, rs_bufs[g].at[k - 1], rs_send.at[g], rs_recv.at[g], {"ty": there})

    def ag_copy(g, k):
        half, span_rows = sizes(g)
        there = (ty + k) % n_ty
        dst = ag_bufs[g].at[pl.ds(pl.multiple_of(tx * half + ty * span_rows, 8), span_rows), :]
        return copy_to(sums[g], dst, ag_send.at[g], ag_recv.at[g], {"ty": there})

    def scatter(g):
        half, _ = sizes(g)
        swap_copy(g).wait_recv()
        chip_sums[g][...] = modes[g][pl.ds(pl.multiple_of(tx * half, 8), half), :] + swapped[g][...]
        for k in range(1, n_ty):
            rs_copy(g, k).start()

    def reduce(g):
        half, span_rows = sizes(g)
        whole = rs_bufs[g]
        copy_to(whole, whole, rs_send.at[g], rs_recv.at[g], {"tx": mate}).wait_recv()
        part = chip_sums[g][pl.ds(pl.multiple_of(ty * span_rows, 8), span_rows), :]
        total = part + jnp.sum(rs_bufs[g][...], axis=0)
        sums[g][...] = total
        for k in range(1, n_ty):
            ag_copy(g, k).start()
        ag_bufs[g][pl.ds(pl.multiple_of(tx * half + ty * span_rows, 8), span_rows), :] = total

    def hand_back(g):
        whole = rs_bufs[g]
        copy_to(whole, whole, ag_send.at[g], ag_recv.at[g], {"tx": mate}).wait_recv()
        back_copy(g).start()

    def nudge(g):
        half, _ = sizes(g)
        ref = ag_bufs[g].at[pl.ds(pl.multiple_of(mate * half, 8), half), :]
        copy_to(ref, ref, back_send.at[g], back_recv.at[g], {"tx": mate}).wait_recv()
        for f in groups[g]:
            coef = ag_bufs[g][pl.ds((f - groups[g][0]) * 128, 128), :]
            term = relaxation[f] * (driver[f] - coef)
            recon = jnp.dot(row_b[...], term, precision=HI, preferred_element_type=jnp.float32)
            for start in range(0, cols, 2 * BS):
                span = slice(start, start + 2 * BS)
                out[f, :, span] += lax.dot_general(
                    recon, col_b[span, :], (((1,), (1,)), ((), ())), precision=HI, preferred_element_type=jnp.float32)

    last_chunk = {f: c for c, (f, _, _, _) in enumerate(chunks)}
    group_of = {f: g for g, fs in enumerate(groups) for f in fs}
    todo = {}

    def finish(c, k):
        blend(c)
        f = chunks[c][0]
        if last_chunk[f] == c:
            g = group_of[f]
            project(g, f)
            if f == groups[g][-1]:
                due = k
                for step, gap in zip((scatter, reduce, hand_back, nudge), ADDS):
                    due += gap
                    todo.setdefault(due, []).append((step, g))

    started = 0
    while started < min(LAUNCH, n_chunks):
        launch(started)
        started += 1
    mine_copy.wait()
    fresh = list(range(n_fields))
    tendency(fresh.pop(0))
    k = 0
    while k < n_chunks + FINISH or todo:
        if k == 1:
            for copy in tabs:
                copy.wait()
            for copy in want[0]:
                copy.wait_recv()

            @pl.when(inner)
            def _():
                for copy in want[1]:
                    copy.wait_recv()
        if k < n_chunks:
            first_hop(k)
        if started < n_chunks:
            launch(started)
            started += 1
        if 0 <= k - SECOND < n_chunks:
            second_hop(k - SECOND)
        if 0 <= k - COLLECT < n_chunks:
            collect(k - COLLECT)
        if 0 <= k - ANSWER < n_chunks:
            answer(k - ANSWER)
        if fresh:
            tendency(fresh.pop(0))
        for step, g in todo.pop(k, ()):
            step(g)
        if 0 <= k - FINISH < n_chunks:
            finish(k - FINISH, k)
        k += 1

    for c in range(n_chunks):
        mode = chunks[c][3]

        @pl.when(inner)
        def _():
            ref = gathered[c].at[pl.ds(0, 7 * per_tile)]
            copy_to(ref, ref, sent.at[c], recv.at[c, 0], {"ty": rung}).wait_send()
            if mode == "P":
                to_mate(c, column(c, tx)).wait_send()

        @pl.when(end)
        def _():
            ref = gathered[c].at[pl.ds(0, 3 * per_tile)]
            copy_to(ref, ref, sent.at[c], recv.at[c, 0], {"ty": rung}).wait_send()

        if mode == "Q":
            to_mate(c, rail(c, tx)).wait_send()
    for copy in want[0]:
        copy.wait_send()

    @pl.when(end)
    def _():
        for copy in want[1]:
            copy.wait_send()
    for g in range(n_groups):
        swap_copy(g).wait_send()
        back_copy(g).wait_send()
        whole = rs_bufs[g]
        copy_to(whole, whole, rs_send.at[g], rs_recv.at[g], {"tx": mate}).wait_send()
        copy_to(whole, whole, ag_send.at[g], ag_recv.at[g], {"tx": mate}).wait_send()


def ladder_call(
    n_ty, n_tx, fields, weights, tile, block, coupling, driver, relaxation, row_tab, row_tab_t, col_tab,
):
    n_fields, rows, cols = fields.shape
    chunks, groups = ladder_plan(n_fields, rows)
    n_chunks, n_groups = len(chunks), len(groups)
    per_tile = cols // BS
    vmem = pl.BlockSpec(memory_space=pltpu.VMEM)
    smem = pl.BlockSpec(memory_space=pltpu.SMEM)
    hbm = pl.BlockSpec(memory_space=pltpu.HBM)
    dma = pltpu.SemaphoreType.DMA
    halves = [len(g) * 128 // n_tx for g in groups]
    asks = pltpu.SMEM((2, per_tile), jnp.int32)
    scratch = (
        [pltpu.VMEM((n_ty * n_tx * per_tile, c[2], BS), jnp.bfloat16) for c in chunks]
        + [pltpu.VMEM((2 * per_tile, c[2], BS), jnp.bfloat16) for c in chunks] * 2
        + [pltpu.VMEM((len(g) * 128, 128), jnp.float32) for g in groups]
        + [pltpu.VMEM((h, 128), jnp.float32) for h in halves] * 2
        + [pltpu.VMEM((n_ty - 1, h // n_ty, 128), jnp.float32) for h in halves]
        + [pltpu.VMEM((h // n_ty, 128), jnp.float32) for h in halves]
        + [pltpu.VMEM((len(g) * 128, 128), jnp.float32) for g in groups]
        + [
            pltpu.VMEM((rows, 128), jnp.float32),
            pltpu.VMEM((128, rows), jnp.float32),
            pltpu.VMEM((cols, 128), jnp.float32),
            pltpu.VMEM((rows, cols), jnp.bfloat16),
            pltpu.VMEM(driver.shape, jnp.float32),
            pltpu.VMEM(relaxation.shape, jnp.float32),
            pltpu.VMEM(fields.shape, jnp.bfloat16),
            asks, asks, asks, asks,
            dma((6,)),
            dma((n_chunks, per_tile)),
            dma,
            dma((4,)),
            dma((4,)),
            dma((n_chunks,)),
            dma((n_chunks, 9)),
            dma((n_chunks,)),
            dma((n_chunks,)),
            *[dma((n_groups,))] * 8,
        ]
    )
    return pl.pallas_call(
        functools.partial(ladder_kernel, n_ty, n_tx, chunks, groups),
        out_shape=jax.ShapeDtypeStruct((n_fields, rows, cols), jnp.float32),
        in_specs=[hbm, hbm, smem, smem, vmem, hbm, hbm, hbm, hbm, hbm],
        out_specs=vmem,
        scratch_shapes=scratch,
        compiler_params=pltpu.CompilerParams(
            collective_id=0, has_side_effects=True, vmem_limit_bytes=67043328
        ),
        name="remap_ladder",
    )(fields, weights, tile, block, coupling, driver, relaxation, row_tab, row_tab_t, col_tab)


def solution(mesh):
    n_ty, n_tx = mesh.shape["ty"], mesh.shape["tx"]
    snake = two_lines(mesh)
    rungs = ladder(mesh)

    def body(fields, weights, source_tile, source_block, coupling, driver, relaxation):
        n_fields, rows, cols = fields.shape
        n_groups = n_fields // GROUP
        n_dev = n_ty * n_tx
        half = GROUP * 128 // n_tx
        span_rows = half // n_ty
        row_np, col_np = wave_table(rows * n_ty), wave_table(cols * n_tx)
        row_tab, row_tab_t = jnp.asarray(row_np), jnp.asarray(np.ascontiguousarray(row_np.T))
        if row_np.shape == col_np.shape:
            col_tab = row_tab
        else:
            col_tab = jnp.asarray(col_np)
        tile = jnp.transpose(source_tile, (0, 2, 1))[0]
        block = jnp.transpose(source_block, (0, 2, 1))[0]
        if rungs:
            return ladder_call(
                n_ty, n_tx, fields, weights, tile, block, coupling, driver, relaxation, row_tab, row_tab_t, col_tab)
        picks = (tile % n_tx * n_ty + tile // n_tx) * (cols // BS) + block
        vmem = pl.BlockSpec(memory_space=pltpu.VMEM)
        smem = pl.BlockSpec(memory_space=pltpu.SMEM)
        hbm = pl.BlockSpec(memory_space=pltpu.HBM)
        dma = pltpu.SemaphoreType.DMA
        scratch = (
            [pltpu.VMEM((n_dev * (cols // BS), BS, BS), jnp.bfloat16)] * n_fields
            + [pltpu.VMEM((GROUP * 128, 128), jnp.float32)] * n_groups
            + [pltpu.VMEM((half, 128), jnp.float32)] * (2 * n_groups)
            + [pltpu.VMEM((n_ty - 1, span_rows, 128), jnp.float32)] * n_groups
            + [pltpu.VMEM((span_rows, 128), jnp.float32)] * n_groups
            + [pltpu.VMEM((GROUP * 128, 128), jnp.float32)] * n_groups
            + [
                pltpu.VMEM((rows, 128), jnp.float32),
                pltpu.VMEM((128, rows), jnp.float32),
                pltpu.VMEM((cols, 128), jnp.float32),
                pltpu.VMEM((rows, cols), jnp.bfloat16),
                pltpu.VMEM(driver.shape, jnp.float32),
                pltpu.VMEM(relaxation.shape, jnp.float32),
                dma((6,)),
                dma((n_fields, cols // BS)),
                dma((n_fields,)),
                dma((n_fields, 2, 2, n_ty // 2)),
                dma((n_fields,)),
                dma((n_fields,)),
                *[dma((n_groups,))] * 8,
            ]
        )
        return pl.pallas_call(
            functools.partial(ring_kernel, n_ty, n_tx, snake),
            out_shape=jax.ShapeDtypeStruct((n_fields, rows, cols), jnp.float32),
            in_specs=[hbm, hbm, smem, vmem, hbm, hbm, hbm, hbm, hbm],
            out_specs=vmem,
            scratch_shapes=scratch,
            compiler_params=pltpu.CompilerParams(
                collective_id=0, has_side_effects=True, vmem_limit_bytes=67043328
            ),
            name="remap_nudge",
        )(fields, weights, picks, coupling, driver, relaxation, row_tab, row_tab_t, col_tab)

    in_specs = (
        P(None, ("groups", "ty"), "tx"),
        P(("groups", "ty"), "tx"),
        P(("groups", "ty"), "tx", None),
        P(("groups", "ty"), "tx", None),
        P(),
        P(),
        P(),
    )
    out_specs = P(None, ("groups", "ty"), "tx")
    return jax.shard_map(body, mesh=mesh, in_specs=in_specs, out_specs=out_specs, check_vma=False)
```

```python
import functools
import math

import jax
import jax.numpy as jnp
import numpy as np
from jax import lax
from jax.experimental import pallas as pl
from jax.experimental.pallas import tpu as pltpu
from jax.sharding import PartitionSpec as P

BS = 128
KMAX = 64
GROUP = 2
MESH = pl.DeviceIdType.MESH
HI = lax.Precision.HIGHEST


def wave_table(period):
    position = np.arange(period, dtype=np.int64)[:, None]
    mode = np.arange(KMAX, dtype=np.int64)[None, :]
    norming = np.where(mode == 0, math.sqrt(1.0 / period), math.sqrt(2.0 / period))
    cos_part = np.cos(2.0 * math.pi * (position * mode % period) / period) * norming
    sin_part = np.sin(2.0 * math.pi * (position * (mode + 1) % period) / period) * math.sqrt(2.0 / period)
    return np.concatenate([cos_part, sin_part], axis=1).astype(np.float32)


def two_lines(mesh):
    devices = np.asarray(mesh.devices)
    axis = list(mesh.axis_names).index("ty")
    line = np.moveaxis(devices, axis, 0).reshape(devices.shape[axis], -1)[:, 0]
    coords = [getattr(d, "coords", None) for d in line]
    if any(c is None for c in coords) or len(line) % 2:
        return False
    varying = [k for k in range(len(coords[0])) if len({c[k] for c in coords}) > 1]
    return len(varying) > 1


def ring_kernel(
    n_ty, n_tx, snake,
    fields, weights_hbm, picks, coupling, driver_hbm, relaxation_hbm, row_tab, row_tab_t, col_tab,
    out, *scratch,
):
    n_fields, rows, cols = fields.shape
    gathered = scratch[:n_fields]
    n_groups = n_fields // GROUP
    (modes, swapped, chip_sums, rs_bufs, sums, ag_bufs) = (
        scratch[n_fields + k * n_groups : n_fields + (k + 1) * n_groups] for k in range(6))
    (row_b, row_bt, col_b, weights, driver, relaxation, tab_sem, own_sem, ring_send, ring_recv, mate_send, mate_recv,
     rs_send, rs_recv, ag_send, ag_recv, swap_send, swap_recv, back_send, back_recv) = scratch[n_fields + 6 * n_groups :]
    per_tile = cols // BS
    ty = lax.axis_index("ty")
    tx = lax.axis_index("tx")
    mate = 1 - tx
    depth = n_ty // 2

    def ring_to_ty(pos):
        pos = (pos + n_ty) % n_ty
        if not snake:
            return pos
        return jnp.where(pos < n_ty // 2, 2 * pos, 2 * (n_ty - 1 - pos) + 1)

    ring = jnp.where(ty % 2 == 0, ty // 2, n_ty - 1 - ty // 2) if snake else ty
    toward = (ring_to_ty(ring + 1), ring_to_ty(ring - 1))

    tabs = [
        pltpu.make_async_copy(row_tab.at[pl.ds(ty * rows, rows), :], row_b, tab_sem.at[0]),
        pltpu.make_async_copy(row_tab_t.at[:, pl.ds(pl.multiple_of(ty * rows, 128), rows)], row_bt, tab_sem.at[1]),
        pltpu.make_async_copy(col_tab.at[pl.ds(tx * cols, cols), :], col_b, tab_sem.at[2]),
        pltpu.make_async_copy(weights_hbm, weights, tab_sem.at[3]),
        pltpu.make_async_copy(driver_hbm, driver, tab_sem.at[4]),
        pltpu.make_async_copy(relaxation_hbm, relaxation, tab_sem.at[5]),
    ]

    def tile_of(f, col, row, part=None):
        first, count = (col * n_ty + row) * per_tile, per_tile
        if part is not None:
            count = per_tile // 2
            first = first + part * count
        return gathered[f].at[pl.ds(first, count)]

    def column_of(f, col):
        return gathered[f].at[pl.ds(col * n_ty * per_tile, n_ty * per_tile)]

    barrier = pltpu.get_barrier_semaphore()
    pl.semaphore_signal(barrier, inc=1, device_id={"tx": mate}, device_id_type=MESH)
    for k in range(1, n_ty):
        pl.semaphore_signal(barrier, inc=1, device_id={"ty": (ty + k) % n_ty}, device_id_type=MESH)
    here = (tx * n_ty + ty) * per_tile

    own = [
        pltpu.make_async_copy(fields.at[f, :, pl.ds(b * BS, BS)], gathered[f].at[here + b], own_sem.at[f, b])
        for f in range(n_fields)
        for b in range(per_tile)
    ]
    for copy in own + tabs:
        copy.start()
    pl.semaphore_wait(barrier, n_ty)
    for copy in own:
        copy.wait()

    def to_mate(f, ref):
        return pltpu.make_async_remote_copy(
            src_ref=ref, dst_ref=ref, send_sem=mate_send.at[f], recv_sem=mate_recv.at[f],
            device_id={"tx": mate}, device_id_type=MESH)

    def sign(way):
        return 1 if way == 0 else -1

    def travels(way, h, d):
        return d < depth - 1 or (d == depth - 1 and h == way)

    def ring_copy(f, way, h, d):
        ref = tile_of(f, tx, ring_to_ty(ring - sign(way) * d), h)
        return pltpu.make_async_remote_copy(
            src_ref=ref, dst_ref=ref,
            send_sem=ring_send.at[f], recv_sem=ring_recv.at[f, way, h, d],
            device_id={"ty": toward[way]}, device_id_type=MESH)

    def arrived(f, way, h, d):
        ref = tile_of(f, tx, ring_to_ty(ring - sign(way) * (d + 1)), h)
        pltpu.make_async_remote_copy(
            src_ref=ref, dst_ref=ref, send_sem=ring_send.at[f], recv_sem=ring_recv.at[f, way, h, d],
            device_id={"ty": toward[way]}, device_id_type=MESH).wait_recv()
        return ref

    def stage(g, d):
        for f in range(g * GROUP, (g + 1) * GROUP):
            for h in range(2):
                for way in range(2):
                    came = d > 0 and travels(way, h, d - 1)
                    if came:
                        got = arrived(f, way, h, d - 1)
                    if travels(way, h, d):
                        ring_copy(f, way, h, d).start()
                    if came:
                        to_mate(f, got).start()
            if d == 0:
                to_mate(f, tile_of(f, tx, ty)).start()

    def tendency(g):
        for f in range(g * GROUP, (g + 1) * GROUP):
            for b in range(per_tile):
                span = slice(b * BS, (b + 1) * BS)
                total = coupling[f : f + 1, 0:1].astype(jnp.float32) * gathered[0][here + b].astype(jnp.float32)
                for k in range(1, n_fields):
                    total = total + coupling[f : f + 1, k : k + 1].astype(jnp.float32) * gathered[k][here + b].astype(jnp.float32)
                out[f, :, span] = total

    def upstream(g):
        for f in range(g * GROUP, (g + 1) * GROUP):
            to_mate(f, column_of(f, mate)).wait_recv()
            for j in range(per_tile):
                span = slice(j * BS, (j + 1) * BS)

                first = gathered[f][picks[0, j]].astype(jnp.float32)
                second = gathered[f][picks[1, j]].astype(jnp.float32)
                w = weights[:, span].astype(jnp.float32)
                out[f, :, span] = out[f, :, span] + (w * first + (1.0 - w) * second)
            col_modes = jnp.zeros((rows, 128), jnp.float32)
            for start in range(0, cols, 2 * BS):
                span = slice(start, start + 2 * BS)
                col_modes += jnp.dot(out[f, :, span], col_b[span, :], precision=HI, preferred_element_type=jnp.float32)
            part = jnp.dot(row_bt[...], col_modes, precision=HI, preferred_element_type=jnp.float32)
            modes[g][pl.ds((f - g * GROUP) * 128, 128), :] = part
        swap_copy(g).start()

    half = GROUP * 128 // n_tx
    span_rows = half // n_ty

    def half_copy(src, dst, send, recv):
        return pltpu.make_async_remote_copy(
            src_ref=src, dst_ref=dst, send_sem=send, recv_sem=recv, device_id={"tx": mate}, device_id_type=MESH)

    def swap_copy(g):
        src = modes[g].at[pl.ds(pl.multiple_of(mate * half, 8), half), :]
        return half_copy(src, swapped[g], swap_send.at[g], swap_recv.at[g])

    def back_copy(g):
        ref = ag_bufs[g].at[pl.ds(pl.multiple_of(tx * half, 8), half), :]
        return half_copy(ref, ref, back_send.at[g], back_recv.at[g])

    def rs_copy(g, k):
        there = (ty + k) % n_ty
        return pltpu.make_async_remote_copy(
            src_ref=chip_sums[g].at[pl.ds(pl.multiple_of(there * span_rows, 8), span_rows), :], dst_ref=rs_bufs[g].at[k - 1],
            send_sem=rs_send.at[g], recv_sem=rs_recv.at[g], device_id={"ty": there}, device_id_type=MESH)

    def ag_copy(g, k):
        there = (ty + k) % n_ty
        return pltpu.make_async_remote_copy(
            src_ref=sums[g], dst_ref=ag_bufs[g].at[pl.ds(pl.multiple_of(tx * half + ty * span_rows, 8), span_rows), :],
            send_sem=ag_send.at[g], recv_sem=ag_recv.at[g], device_id={"ty": there}, device_id_type=MESH)

    def scatter(g):
        swap_copy(g).wait_recv()
        chip_sums[g][...] = modes[g][pl.ds(pl.multiple_of(tx * half, 8), half), :] + swapped[g][...]
        for k in range(1, n_ty):
            rs_copy(g, k).start()

    def reduce(g):
        whole = rs_bufs[g]
        half_copy(whole, whole, rs_send.at[g], rs_recv.at[g]).wait_recv()
        mine = chip_sums[g][pl.ds(pl.multiple_of(ty * span_rows, 8), span_rows), :]
        total = mine + jnp.sum(rs_bufs[g][...], axis=0)
        sums[g][...] = total
        for k in range(1, n_ty):
            ag_copy(g, k).start()
        ag_bufs[g][pl.ds(pl.multiple_of(tx * half + ty * span_rows, 8), span_rows), :] = total

    def hand_back(g):
        whole = rs_bufs[g]
        half_copy(whole, whole, ag_send.at[g], ag_recv.at[g]).wait_recv()
        back_copy(g).start()

    def nudge(g):
        ref = ag_bufs[g].at[pl.ds(pl.multiple_of(mate * half, 8), half), :]
        half_copy(ref, ref, back_send.at[g], back_recv.at[g]).wait_recv()
        for f in range(g * GROUP, (g + 1) * GROUP):
            coef = ag_bufs[g][pl.ds((f - g * GROUP) * 128, 128), :]
            term = relaxation[f] * (driver[f] - coef)
            recon = jnp.dot(row_b[...], term, precision=HI, preferred_element_type=jnp.float32)
            for start in range(0, cols, 2 * BS):
                span = slice(start, start + 2 * BS)
                out[f, :, span] += lax.dot_general(
                    recon, col_b[span, :], (((1,), (1,)), ((), ())), precision=HI, preferred_element_type=jnp.float32)

    stage(0, 0)
    for g in range(n_groups):
        tendency(g)
    for copy in tabs:
        copy.wait()
    end = n_groups - 1
    for g in range(end):
        behind = [upstream, scatter, reduce] if g > 0 else []
        for d in range(1, depth):
            stage(g, d)
            if behind:
                behind.pop(0)(g - 1)
        stage(g + 1, 0)
        stage(g, depth)
        if g > 0:
            for step in behind + [hand_back, nudge]:
                step(g - 1)
    for d in range(1, depth):
        stage(end, d)
        if d == 1:
            upstream(end - 1)
    scatter(end - 1)
    stage(end, depth)
    reduce(end - 1)
    upstream(end)
    scatter(end)
    hand_back(end - 1)
    reduce(end)
    nudge(end - 1)
    hand_back(end)
    nudge(end)

    for f in range(n_fields):
        sent = gathered[f].at[pl.ds(0, (n_ty - 1) * per_tile)]
        pltpu.make_async_remote_copy(
            src_ref=sent, dst_ref=sent, send_sem=ring_send.at[f], recv_sem=ring_recv.at[f, 0, 0, 0],
            device_id={"ty": toward[0]}, device_id_type=MESH).wait_send()
        to_mate(f, column_of(f, tx)).wait_send()
    for g in range(n_groups):
        swap_copy(g).wait_send()
        back_copy(g).wait_send()
        whole = rs_bufs[g]
        half_copy(whole, whole, rs_send.at[g], rs_recv.at[g]).wait_send()
        half_copy(whole, whole, ag_send.at[g], ag_recv.at[g]).wait_send()


def ladder(mesh):
    devices = np.asarray(mesh.devices)
    axis = list(mesh.axis_names).index("ty")
    line = np.moveaxis(devices, axis, 0).reshape(devices.shape[axis], -1)[:, 0]
    coords = [getattr(d, "coords", None) for d in line]
    if len(line) != 8 or mesh.shape["tx"] != 2 or any(c is None for c in coords):
        return False
    steps = [[b - a for a, b in zip(coords[0], c)] for c in coords]
    rung, rail = steps[1], steps[2]
    unit = sum(abs(v) for v in rung) == 1 and sum(abs(v) for v in rail) == 1
    return unit and all(
        s == [k // 2 * v + k % 2 * w for v, w in zip(rail, rung)] for k, s in enumerate(steps))


SPLIT = 2
PATTERN = "PQPPQPPQPPQP"
LAUNCH, SECOND, COLLECT, ANSWER, FINISH = 3, 1, 2, 3, 5
ADDS = ((1, 2, 1, 1), (1, 3))
GROUPS = (5, 1)


def ladder_plan(n_fields, rows):
    pieces = SPLIT if rows % (16 * SPLIT) == 0 else 1
    size = rows // pieces
    spots = [(f, r) for f in range(n_fields) for r in range(0, rows, size)]
    chunks = [(f, r, size, PATTERN[k % len(PATTERN)]) for k, (f, r) in enumerate(spots)]
    counts = GROUPS if sum(GROUPS) == n_fields else (1,) * n_fields
    ends = [sum(counts[: k + 1]) for k in range(len(counts))]
    groups = [tuple(range(e - n, e)) for e, n in zip(ends, counts)]
    return tuple(chunks), tuple(groups)


def ladder_kernel(
    n_ty, n_tx, chunks, groups,
    fields, weights_hbm, tile_s, block_s, coupling, driver_hbm, relaxation_hbm, row_tab, row_tab_t, col_tab,
    out, *scratch,
):
    n_fields, rows, cols = fields.shape
    n_chunks, n_groups = len(chunks), len(groups)
    gathered, asked, slots = (scratch[k * n_chunks : (k + 1) * n_chunks] for k in range(3))
    scratch = scratch[3 * n_chunks :]
    (modes, swapped, chip_sums, rs_bufs, sums, ag_bufs) = (
        scratch[k * n_groups : (k + 1) * n_groups] for k in range(6))
    (row_b, row_bt, col_b, weights, driver, relaxation, mine, rung_tile, rung_block, outer_tile, outer_block,
     tab_sem, own_sem, mine_sem, want_send, want_recv, sent, recv, mate_send, mate_recv,
     rs_send, rs_recv, ag_send, ag_recv, swap_send, swap_recv, back_send, back_recv) = scratch[6 * n_groups :]
    per_tile = cols // BS
    n_z = n_ty // 2
    n_ask = 2 * per_tile
    ty = lax.axis_index("ty")
    tx = lax.axis_index("tx")
    mate = 1 - tx
    z, y = ty // 2, ty % 2
    far_y = 1 - y
    left = z < n_z // 2
    end = (z == 0) | (z == n_z - 1)
    inner = jnp.logical_not(end)
    z_end = jnp.where(left, 0, n_z - 1)
    z_in = jnp.where(left, 1, n_z - 2)
    far_end, far_in = n_z - 1 - z_end, n_z - 1 - z_in
    rung = 2 * z + far_y
    across = 2 * far_in + y
    outer = 2 * z_end + y
    inward = 2 * z_in + y

    def copy_to(src, dst, send, got, where):
        return pltpu.make_async_remote_copy(
            src_ref=src, dst_ref=dst, send_sem=send, recv_sem=got, device_id=where, device_id_type=MESH)

    def tile(c, zz, yy, part=None, col=None):
        first, count = ((tx if col is None else col) * n_ty + yy * n_z + zz) * per_tile, per_tile
        if part is not None:
            count = per_tile // 2
            first = first + part * count
        return gathered[c].at[pl.ds(first, count)]

    def rail(c, col):
        return gathered[c].at[pl.ds((col * n_ty + y * n_z) * per_tile, n_z * per_tile)]

    def column(c, col):
        return gathered[c].at[pl.ds(col * n_ty * per_tile, n_ty * per_tile)]

    def send(c, ref, there, kind):
        copy_to(ref, ref, sent.at[c], recv.at[c, kind], {"ty": there}).start()

    def take(c, ref, kind):
        copy_to(ref, ref, sent.at[c], recv.at[c, kind], {"ty": rung}).wait_recv()

    def to_mate(c, ref):
        return copy_to(ref, ref, mate_send.at[c], mate_recv.at[c], {"tx": mate})

    E_OWN, E_FAR, I_ACROSS, E_ACROSS, I_PART, OWN_RUNG, E_RUNG, I_REST, ASKED = range(9)

    tabs = [
        pltpu.make_async_copy(row_tab.at[pl.ds(ty * rows, rows), :], row_b, tab_sem.at[0]),
        pltpu.make_async_copy(row_tab_t.at[:, pl.ds(pl.multiple_of(ty * rows, 128), rows)], row_bt, tab_sem.at[1]),
        pltpu.make_async_copy(col_tab.at[pl.ds(tx * cols, cols), :], col_b, tab_sem.at[2]),
        pltpu.make_async_copy(weights_hbm, weights, tab_sem.at[3]),
        pltpu.make_async_copy(driver_hbm, driver, tab_sem.at[4]),
        pltpu.make_async_copy(relaxation_hbm, relaxation, tab_sem.at[5]),
    ]

    barrier = pltpu.get_barrier_semaphore()
    pl.semaphore_signal(barrier, inc=1, device_id={"tx": mate}, device_id_type=MESH)
    pl.semaphore_signal(barrier, inc=1, device_id={"ty": rung}, device_id_type=MESH)

    @pl.when(inner)
    def _():
        pl.semaphore_signal(barrier, inc=1, device_id={"ty": across}, device_id_type=MESH)
        pl.semaphore_signal(barrier, inc=1, device_id={"ty": outer}, device_id_type=MESH)

    @pl.when(end)
    def _():
        pl.semaphore_signal(barrier, inc=1, device_id={"ty": inward}, device_id_type=MESH)
    here = (tx * n_ty + y * n_z + z) * per_tile
    own = [
        [pltpu.make_async_copy(fields.at[f, pl.ds(r0, nr), pl.ds(b * BS, BS)], gathered[c].at[here + b], own_sem.at[c, b])
         for b in range(per_tile)]
        for c, (f, r0, nr, _) in enumerate(chunks)
    ]
    mine_copy = pltpu.make_async_copy(fields, mine, mine_sem)
    for copies in own:
        for copy in copies:
            copy.start()
    for copy in [mine_copy] + tabs:
        copy.start()

    @pl.when(inner)
    def _():
        pl.semaphore_wait(barrier, 4)

    @pl.when(end)
    def _():
        pl.semaphore_wait(barrier, 3)

    want = [
        (copy_to(tile_s, rung_tile, want_send.at[0], want_recv.at[0], {"ty": rung}),
         copy_to(block_s, rung_block, want_send.at[1], want_recv.at[1], {"ty": rung})),
        (copy_to(tile_s, outer_tile, want_send.at[2], want_recv.at[2], {"ty": inward}),
         copy_to(block_s, outer_block, want_send.at[3], want_recv.at[3], {"ty": inward})),
    ]
    for copy in want[0]:
        copy.start()

    @pl.when(end)
    def _():
        for copy in want[1]:
            copy.start()

    def spot(tiles, blocks, s, j):
        t = tiles[s, j]
        row, col = lax.div(t, n_tx), lax.rem(t, n_tx)
        row_z, row_y = lax.div(row, 2), lax.rem(row, 2)
        return col, row_z, row_y, blocks[s, j]

    def place(col, row_z, row_y, block):
        return (col * n_ty + row_y * n_z + row_z) * per_tile + block

    def launch(c):
        for copy in own[c]:
            copy.wait()
        ref = tile(c, z, y)
        if chunks[c][3] == "P":
            @pl.when(inner)
            def _():
                send(c, ref, rung, OWN_RUNG)
                send(c, ref, across, I_ACROSS)
                to_mate(c, ref).start()

            @pl.when(end)
            def _():
                send(c, ref, rung, OWN_RUNG)
                send(c, ref, inward, E_OWN)
        else:
            @pl.when(inner)
            def _():
                send(c, ref, across, I_ACROSS)
                send(c, ref, outer, E_OWN)

            @pl.when(end)
            def _():
                send(c, ref, inward, E_OWN)
            to_mate(c, ref).start()

    def first_hop(c):
        if chunks[c][3] == "P":
            @pl.when(inner)
            def _():
                ref = tile(c, z_end, y)
                take(c, ref, E_OWN)
                send(c, ref, across, E_ACROSS)
                to_mate(c, ref).start()
                ref = tile(c, z, far_y)
                take(c, ref, OWN_RUNG)
                send(c, tile(c, z, far_y, 0), across, I_PART)
                to_mate(c, ref).start()
                ref = tile(c, far_in, y)
                take(c, ref, I_ACROSS)
                send(c, tile(c, far_in, y, 1), rung, I_REST)
                to_mate(c, ref).start()

            @pl.when(end)
            def _():
                ref = tile(c, z, far_y)
                take(c, ref, OWN_RUNG)
                send(c, ref, inward, E_FAR)
        else:
            @pl.when(inner)
            def _():
                ref = tile(c, z_end, y)
                take(c, ref, E_OWN)
                send(c, ref, across, E_ACROSS)
                to_mate(c, ref).start()
                ref = tile(c, far_in, y)
                take(c, ref, I_ACROSS)
                send(c, ref, outer, I_ACROSS)
                to_mate(c, ref).start()

            @pl.when(end)
            def _():
                ref = tile(c, z_in, y)
                take(c, ref, E_OWN)
                to_mate(c, ref).start()

    def second_hop(c):
        if chunks[c][3] == "P":
            @pl.when(inner)
            def _():
                ref = tile(c, far_end, y)
                take(c, ref, E_ACROSS)
                send(c, ref, rung, E_RUNG)
                to_mate(c, ref).start()
                ref = tile(c, z_end, far_y)
                take(c, ref, E_FAR)
                to_mate(c, ref).start()
        else:
            @pl.when(inner)
            def _():
                ref = tile(c, far_end, y)
                take(c, ref, E_ACROSS)
                send(c, ref, outer, E_ACROSS)
                to_mate(c, ref).start()

            @pl.when(end)
            def _():
                ref = tile(c, far_in, y)
                take(c, ref, I_ACROSS)
                to_mate(c, ref).start()

    def collect(c):
        if chunks[c][3] == "P":
            @pl.when(inner)
            def _():
                take(c, tile(c, far_in, far_y, 0), I_PART)
                take(c, tile(c, far_in, far_y, 1), I_REST)
                to_mate(c, tile(c, far_in, far_y)).start()
                ref = tile(c, far_end, far_y)
                take(c, ref, E_RUNG)
                to_mate(c, ref).start()
        else:
            @pl.when(end)
            def _():
                ref = tile(c, far_end, y)
                take(c, ref, E_ACROSS)
                to_mate(c, ref).start()

    def answer(c):
        if chunks[c][3] == "P":
            @pl.when(inner)
            def _():
                to_mate(c, column(c, mate)).wait_recv()
                for s in range(2):
                    for j in range(per_tile):
                        col, row_z, row_y, block = spot(outer_tile, outer_block, s, j)
                        asked[c][s * per_tile + j] = gathered[c][place(col, row_z, row_y, block)]
                copy_to(asked[c], slots[c], sent.at[c], recv.at[c, ASKED], {"ty": outer}).start()
        else:
            to_mate(c, rail(c, mate)).wait_recv()
            for s in range(2):
                for j in range(per_tile):
                    col, row_z, row_y, block = spot(rung_tile, rung_block, s, j)
                    asked[c][s * per_tile + j] = gathered[c][place(col, row_z, y, block)]
            copy_to(asked[c], slots[c], sent.at[c], recv.at[c, ASKED], {"ty": rung}).start()

    def blend(c):
        f, r0, nr, mode = chunks[c]
        whole = copy_to(asked[c], slots[c], sent.at[c], recv.at[c, ASKED], {"ty": rung})
        if mode == "P":
            @pl.when(end)
            def _():
                whole.wait_recv()
        else:
            whole.wait_recv()

        def source(s, j):
            col, row_z, row_y, block = spot(tile_s, block_s, s, j)
            if mode == "P":
                here_too = inner
                at = place(col, row_z, row_y, block)
            else:
                here_too = row_y == y
                at = place(col, row_z, y, block)
            return jnp.where(here_too, gathered[c][at].astype(jnp.float32), slots[c][s * per_tile + j].astype(jnp.float32))

        for j in range(per_tile):
            span = slice(j * BS, (j + 1) * BS)
            w = weights[r0 : r0 + nr, span].astype(jnp.float32)
            out[f, r0 : r0 + nr, span] = out[f, r0 : r0 + nr, span] + (w * source(0, j) + (1.0 - w) * source(1, j))

    def tendency(f):
        for b in range(per_tile):
            span = slice(b * BS, (b + 1) * BS)
            total = coupling[f : f + 1, 0:1].astype(jnp.float32) * mine[0, :, span].astype(jnp.float32)
            for k in range(1, n_fields):
                total = total + coupling[f : f + 1, k : k + 1].astype(jnp.float32) * mine[k, :, span].astype(jnp.float32)
            out[f, :, span] = total

    def project(g, f):
        col_modes = jnp.zeros((rows, 128), jnp.float32)
        for start in range(0, cols, 2 * BS):
            span = slice(start, start + 2 * BS)
            col_modes += jnp.dot(out[f, :, span], col_b[span, :], precision=HI, preferred_element_type=jnp.float32)
        part = jnp.dot(row_bt[...], col_modes, precision=HI, preferred_element_type=jnp.float32)
        modes[g][pl.ds((f - groups[g][0]) * 128, 128), :] = part
        if f == groups[g][-1]:
            if g in direct:
                spread(g)
            else:
                swap_copy(g).start()

    direct = (n_groups - 1,)

    def sizes(g):
        half = len(groups[g]) * 128 // n_tx
        return half, half // n_ty

    def rows_of(ref, first, count):
        return ref.at[pl.ds(pl.multiple_of(first, 8), count), :]

    def swap_copy(g):
        half, _ = sizes(g)
        return copy_to(rows_of(modes[g], mate * half, half), swapped[g], swap_send.at[g], swap_recv.at[g], {"tx": mate})

    def back_copy(g):
        half, _ = sizes(g)
        ref = rows_of(ag_bufs[g], tx * half, half)
        return copy_to(ref, ref, back_send.at[g], back_recv.at[g], {"tx": mate})

    def rs_copy(g, k):
        _, span = sizes(g)
        there = (ty + k) % n_ty
        src = rows_of(chip_sums[g], there * span, span)
        return copy_to(src, rs_bufs[g].at[k - 1], rs_send.at[g], rs_recv.at[g], {"ty": there})

    def ag_copy(g, k):
        half, span = sizes(g)
        dst = rows_of(ag_bufs[g], tx * half + ty * span, span)
        return copy_to(sums[g], dst, ag_send.at[g], ag_recv.at[g], {"ty": (ty + k) % n_ty})

    def scatter(g):
        half, _ = sizes(g)
        swap_copy(g).wait_recv()
        chip_sums[g][...] = modes[g][pl.ds(pl.multiple_of(tx * half, 8), half), :] + swapped[g][...]
        for k in range(1, n_ty):
            rs_copy(g, k).start()

    def reduce(g):
        half, span = sizes(g)
        whole = rs_bufs[g]
        copy_to(whole, whole, rs_send.at[g], rs_recv.at[g], {"tx": mate}).wait_recv()
        total = chip_sums[g][pl.ds(pl.multiple_of(ty * span, 8), span), :] + jnp.sum(rs_bufs[g][...], axis=0)
        sums[g][...] = total
        for k in range(1, n_ty):
            ag_copy(g, k).start()
        ag_bufs[g][pl.ds(pl.multiple_of(tx * half + ty * span, 8), span), :] = total

    def hand_back(g):
        whole = rs_bufs[g]
        copy_to(whole, whole, ag_send.at[g], ag_recv.at[g], {"tx": mate}).wait_recv()
        back_copy(g).start()

    def nudge(g):
        half, _ = sizes(g)
        ref = rows_of(ag_bufs[g], mate * half, half)
        copy_to(ref, ref, back_send.at[g], back_recv.at[g], {"tx": mate}).wait_recv()
        correct(g)

    def correct(g):
        for f in groups[g]:
            coef = ag_bufs[g][pl.ds((f - groups[g][0]) * 128, 128), :]
            term = relaxation[f] * (driver[f] - coef)
            recon = jnp.dot(row_b[...], term, precision=HI, preferred_element_type=jnp.float32)
            for start in range(0, cols, 2 * BS):
                span = slice(start, start + 2 * BS)
                out[f, :, span] += lax.dot_general(
                    recon, col_b[span, :], (((1,), (1,)), ((), ())), precision=HI, preferred_element_type=jnp.float32)

    n_own = n_ty * n_tx // 2

    def relations():
        for dz in range(2):
            for dy in range(2):
                for dt in range(2):
                    yield dz * 4 + dy * 2 + dt, (z_in, far_in)[dz], (z_end, far_end)[dz], (y, far_y)[dy], (tx, mate)[dt]

    def owner_rows(g, zz, yy, tt):
        span = len(groups[g]) * 128 // n_own
        return ((zz - 1) * 4 + yy * 2 + tt) * span, span

    def spread_copy(g, slot, zz, yy, tt):
        src = rows_of(modes[g], *owner_rows(g, zz, yy, tt))
        return copy_to(src, rs_bufs[g].at[slot], rs_send.at[g], rs_recv.at[g], {"ty": 2 * zz + yy, "tx": tt})

    def spread(g):
        @pl.when(inner)
        def _():
            for k, zz, _, yy, tt in relations():
                if k:
                    spread_copy(g, k, zz, yy, tt).start()

        @pl.when(end)
        def _():
            for k, zz, _, yy, tt in relations():
                spread_copy(g, n_own + k, zz, yy, tt).start()

    def slices(g, count):
        ref = rs_bufs[g].at[pl.ds(0, count)]
        return copy_to(ref, ref, rs_send.at[g], rs_recv.at[g], {"tx": mate})

    def answers(g, count):
        ref = rs_bufs[g].at[pl.ds(0, count)]
        return copy_to(ref, ref, ag_send.at[g], ag_recv.at[g], {"tx": mate})

    def settle(g):
        @pl.when(inner)
        def _():
            slices(g, 2 * n_own - 1).wait_recv()
            first, span = owner_rows(g, z, y, tx)
            total = modes[g][pl.ds(pl.multiple_of(first, 8), span), :] + jnp.sum(rs_bufs[g][1:], axis=0)
            sums[g][...] = total
            dst = rows_of(ag_bufs[g], first, span)
            for k, zz, ze, yy, tt in relations():
                copy_to(sums[g], dst, ag_send.at[g], ag_recv.at[g], {"ty": 2 * ze + yy, "tx": tt}).start()
                if k:
                    copy_to(sums[g], dst, ag_send.at[g], ag_recv.at[g], {"ty": 2 * zz + yy, "tx": tt}).start()
            ag_bufs[g][pl.ds(pl.multiple_of(first, 8), span), :] = total

    def nudge_direct(g):
        @pl.when(inner)
        def _():
            answers(g, n_own - 1).wait_recv()

        @pl.when(end)
        def _():
            answers(g, n_own).wait_recv()
        correct(g)

    last_chunk = {f: c for c, (f, _, _, _) in enumerate(chunks)}
    group_of = {f: g for g, fs in enumerate(groups) for f in fs}
    todo = {}

    def finish(c, k):
        blend(c)
        f = chunks[c][0]
        if last_chunk[f] == c:
            g = group_of[f]
            project(g, f)
            if f == groups[g][-1]:
                due = k
                steps = (settle, nudge_direct) if g in direct else (scatter, reduce, hand_back, nudge)
                for step, gap in zip(steps, ADDS[g]):
                    due += gap
                    todo.setdefault(due, []).append((step, g))

    started = 0
    while started < min(LAUNCH, n_chunks):
        launch(started)
        started += 1
    mine_copy.wait()
    fresh = list(range(n_fields))
    tendency(fresh.pop(0))
    k = 0
    while k < n_chunks + FINISH or todo:
        if k == 1:
            for copy in tabs:
                copy.wait()
            for copy in want[0]:
                copy.wait_recv()

            @pl.when(inner)
            def _():
                for copy in want[1]:
                    copy.wait_recv()
        if k < n_chunks:
            first_hop(k)
        if started < n_chunks:
            launch(started)
            started += 1
        if 0 <= k - SECOND < n_chunks:
            second_hop(k - SECOND)
        if 0 <= k - COLLECT < n_chunks:
            collect(k - COLLECT)
        if 0 <= k - ANSWER < n_chunks:
            answer(k - ANSWER)
        if fresh:
            tendency(fresh.pop(0))
        for step, g in todo.pop(k, ()):
            step(g)
        if 0 <= k - FINISH < n_chunks:
            finish(k - FINISH, k)
        k += 1

    for c in range(n_chunks):
        mode = chunks[c][3]

        @pl.when(inner)
        def _():
            ref = gathered[c].at[pl.ds(0, 7 * per_tile)]
            copy_to(ref, ref, sent.at[c], recv.at[c, 0], {"ty": rung}).wait_send()
            if mode == "P":
                to_mate(c, column(c, tx)).wait_send()

        @pl.when(end)
        def _():
            ref = gathered[c].at[pl.ds(0, 3 * per_tile)]
            copy_to(ref, ref, sent.at[c], recv.at[c, 0], {"ty": rung}).wait_send()

        if mode == "Q":
            to_mate(c, rail(c, tx)).wait_send()
    for copy in want[0]:
        copy.wait_send()

    @pl.when(end)
    def _():
        for copy in want[1]:
            copy.wait_send()
    for g in range(n_groups):
        if g in direct:
            @pl.when(inner)
            def _():
                slices(g, n_own - 1).wait_send()
                answers(g, 2 * n_own - 1).wait_send()

            @pl.when(end)
            def _():
                slices(g, n_own).wait_send()
        else:
            swap_copy(g).wait_send()
            back_copy(g).wait_send()
            whole = rs_bufs[g]
            copy_to(whole, whole, rs_send.at[g], rs_recv.at[g], {"tx": mate}).wait_send()
            copy_to(whole, whole, ag_send.at[g], ag_recv.at[g], {"tx": mate}).wait_send()


def ladder_call(
    n_ty, n_tx, fields, weights, tile, block, coupling, driver, relaxation, row_tab, row_tab_t, col_tab,
):
    n_fields, rows, cols = fields.shape
    chunks, groups = ladder_plan(n_fields, rows)
    n_chunks, n_groups = len(chunks), len(groups)
    per_tile = cols // BS
    vmem = pl.BlockSpec(memory_space=pltpu.VMEM)
    smem = pl.BlockSpec(memory_space=pltpu.SMEM)
    hbm = pl.BlockSpec(memory_space=pltpu.HBM)
    dma = pltpu.SemaphoreType.DMA
    halves = [len(g) * 128 // n_tx for g in groups]
    asks = pltpu.SMEM((2, per_tile), jnp.int32)
    scratch = (
        [pltpu.VMEM((n_ty * n_tx * per_tile, c[2], BS), jnp.bfloat16) for c in chunks]
        + [pltpu.VMEM((2 * per_tile, c[2], BS), jnp.bfloat16) for c in chunks] * 2
        + [pltpu.VMEM((len(g) * 128, 128), jnp.float32) for g in groups]
        + [pltpu.VMEM((h, 128), jnp.float32) for h in halves] * 2
        + [pltpu.VMEM((n_ty - 1, h // n_ty, 128), jnp.float32) for h in halves[:-1]]
        + [pltpu.VMEM((n_ty * n_tx, 2 * halves[-1] // n_ty, 128), jnp.float32)]
        + [pltpu.VMEM((h // n_ty, 128), jnp.float32) for h in halves[:-1]]
        + [pltpu.VMEM((2 * halves[-1] // n_ty, 128), jnp.float32)]
        + [pltpu.VMEM((len(g) * 128, 128), jnp.float32) for g in groups]
        + [
            pltpu.VMEM((rows, 128), jnp.float32),
            pltpu.VMEM((128, rows), jnp.float32),
            pltpu.VMEM((cols, 128), jnp.float32),
            pltpu.VMEM((rows, cols), jnp.bfloat16),
            pltpu.VMEM(driver.shape, jnp.float32),
            pltpu.VMEM(relaxation.shape, jnp.float32),
            pltpu.VMEM(fields.shape, jnp.bfloat16),
            asks, asks, asks, asks,
            dma((6,)),
            dma((n_chunks, per_tile)),
            dma,
            dma((4,)),
            dma((4,)),
            dma((n_chunks,)),
            dma((n_chunks, 9)),
            dma((n_chunks,)),
            dma((n_chunks,)),
            *[dma((n_groups,))] * 8,
        ]
    )
    return pl.pallas_call(
        functools.partial(ladder_kernel, n_ty, n_tx, chunks, groups),
        out_shape=jax.ShapeDtypeStruct((n_fields, rows, cols), jnp.float32),
        in_specs=[hbm, hbm, smem, smem, vmem, hbm, hbm, hbm, hbm, hbm],
        out_specs=vmem,
        scratch_shapes=scratch,
        compiler_params=pltpu.CompilerParams(
            collective_id=0, has_side_effects=True, vmem_limit_bytes=67043328
        ),
        name="remap_ladder",
    )(fields, weights, tile, block, coupling, driver, relaxation, row_tab, row_tab_t, col_tab)


def solution(mesh):
    n_ty, n_tx = mesh.shape["ty"], mesh.shape["tx"]
    snake = two_lines(mesh)
    rungs = ladder(mesh)

    def body(fields, weights, source_tile, source_block, coupling, driver, relaxation):
        n_fields, rows, cols = fields.shape
        n_groups = n_fields // GROUP
        n_dev = n_ty * n_tx
        half = GROUP * 128 // n_tx
        span_rows = half // n_ty
        row_np, col_np = wave_table(rows * n_ty), wave_table(cols * n_tx)
        row_tab, row_tab_t = jnp.asarray(row_np), jnp.asarray(np.ascontiguousarray(row_np.T))
        if row_np.shape == col_np.shape:
            col_tab = row_tab
        else:
            col_tab = jnp.asarray(col_np)
        tile = jnp.transpose(source_tile, (0, 2, 1))[0]
        block = jnp.transpose(source_block, (0, 2, 1))[0]
        if rungs:
            return ladder_call(
                n_ty, n_tx, fields, weights, tile, block, coupling, driver, relaxation, row_tab, row_tab_t, col_tab)
        picks = (tile % n_tx * n_ty + tile // n_tx) * (cols // BS) + block
        vmem = pl.BlockSpec(memory_space=pltpu.VMEM)
        smem = pl.BlockSpec(memory_space=pltpu.SMEM)
        hbm = pl.BlockSpec(memory_space=pltpu.HBM)
        dma = pltpu.SemaphoreType.DMA
        scratch = (
            [pltpu.VMEM((n_dev * (cols // BS), BS, BS), jnp.bfloat16)] * n_fields
            + [pltpu.VMEM((GROUP * 128, 128), jnp.float32)] * n_groups
            + [pltpu.VMEM((half, 128), jnp.float32)] * (2 * n_groups)
            + [pltpu.VMEM((n_ty - 1, span_rows, 128), jnp.float32)] * n_groups
            + [pltpu.VMEM((span_rows, 128), jnp.float32)] * n_groups
            + [pltpu.VMEM((GROUP * 128, 128), jnp.float32)] * n_groups
            + [
                pltpu.VMEM((rows, 128), jnp.float32),
                pltpu.VMEM((128, rows), jnp.float32),
                pltpu.VMEM((cols, 128), jnp.float32),
                pltpu.VMEM((rows, cols), jnp.bfloat16),
                pltpu.VMEM(driver.shape, jnp.float32),
                pltpu.VMEM(relaxation.shape, jnp.float32),
                dma((6,)),
                dma((n_fields, cols // BS)),
                dma((n_fields,)),
                dma((n_fields, 2, 2, n_ty // 2)),
                dma((n_fields,)),
                dma((n_fields,)),
                *[dma((n_groups,))] * 8,
            ]
        )
        return pl.pallas_call(
            functools.partial(ring_kernel, n_ty, n_tx, snake),
            out_shape=jax.ShapeDtypeStruct((n_fields, rows, cols), jnp.float32),
            in_specs=[hbm, hbm, smem, vmem, hbm, hbm, hbm, hbm, hbm],
            out_specs=vmem,
            scratch_shapes=scratch,
            compiler_params=pltpu.CompilerParams(
                collective_id=0, has_side_effects=True, vmem_limit_bytes=67043328
            ),
            name="remap_nudge",
        )(fields, weights, picks, coupling, driver, relaxation, row_tab, row_tab_t, col_tab)

    in_specs = (
        P(None, ("groups", "ty"), "tx"),
        P(("groups", "ty"), "tx"),
        P(("groups", "ty"), "tx", None),
        P(("groups", "ty"), "tx", None),
        P(),
        P(),
        P(),
    )
    out_specs = P(None, ("groups", "ty"), "tx")
    return jax.shard_map(body, mesh=mesh, in_specs=in_specs, out_specs=out_specs, check_vma=False)
```

```python
import functools
import math

import jax
import jax.numpy as jnp
import numpy as np
from jax import lax
from jax.experimental import pallas as pl
from jax.experimental.pallas import tpu as pltpu
from jax.sharding import PartitionSpec as P

BS = 128
KMAX = 64
GROUP = 2
MESH = pl.DeviceIdType.MESH
HI = lax.Precision.HIGH


def wave_table(period):
    position = np.arange(period, dtype=np.int64)[:, None]
    mode = np.arange(KMAX, dtype=np.int64)[None, :]
    norming = np.where(mode == 0, math.sqrt(1.0 / period), math.sqrt(2.0 / period))
    cos_part = np.cos(2.0 * math.pi * (position * mode % period) / period) * norming
    sin_part = np.sin(2.0 * math.pi * (position * (mode + 1) % period) / period) * math.sqrt(2.0 / period)
    return np.concatenate([cos_part, sin_part], axis=1).astype(np.float32)


def two_lines(mesh):
    devices = np.asarray(mesh.devices)
    axis = list(mesh.axis_names).index("ty")
    line = np.moveaxis(devices, axis, 0).reshape(devices.shape[axis], -1)[:, 0]
    coords = [getattr(d, "coords", None) for d in line]
    if any(c is None for c in coords) or len(line) % 2:
        return False
    varying = [k for k in range(len(coords[0])) if len({c[k] for c in coords}) > 1]
    return len(varying) > 1


def ring_kernel(
    n_ty, n_tx, snake,
    fields, weights_hbm, picks, coupling, driver_hbm, relaxation_hbm, row_tab, row_tab_t, col_tab,
    out, *scratch,
):
    n_fields, rows, cols = fields.shape
    gathered = scratch[:n_fields]
    n_groups = n_fields // GROUP
    (modes, swapped, chip_sums, rs_bufs, sums, ag_bufs) = (
        scratch[n_fields + k * n_groups : n_fields + (k + 1) * n_groups] for k in range(6))
    (row_b, row_bt, col_b, weights, driver, relaxation, tab_sem, own_sem, ring_send, ring_recv, mate_send, mate_recv,
     rs_send, rs_recv, ag_send, ag_recv, swap_send, swap_recv, back_send, back_recv) = scratch[n_fields + 6 * n_groups :]
    per_tile = cols // BS
    ty = lax.axis_index("ty")
    tx = lax.axis_index("tx")
    mate = 1 - tx
    depth = n_ty // 2

    def ring_to_ty(pos):
        pos = (pos + n_ty) % n_ty
        if not snake:
            return pos
        return jnp.where(pos < n_ty // 2, 2 * pos, 2 * (n_ty - 1 - pos) + 1)

    ring = jnp.where(ty % 2 == 0, ty // 2, n_ty - 1 - ty // 2) if snake else ty
    toward = (ring_to_ty(ring + 1), ring_to_ty(ring - 1))

    tabs = [
        pltpu.make_async_copy(row_tab.at[pl.ds(ty * rows, rows), :], row_b, tab_sem.at[0]),
        pltpu.make_async_copy(row_tab_t.at[:, pl.ds(pl.multiple_of(ty * rows, 128), rows)], row_bt, tab_sem.at[1]),
        pltpu.make_async_copy(col_tab.at[pl.ds(tx * cols, cols), :], col_b, tab_sem.at[2]),
        pltpu.make_async_copy(weights_hbm, weights, tab_sem.at[3]),
        pltpu.make_async_copy(driver_hbm, driver, tab_sem.at[4]),
        pltpu.make_async_copy(relaxation_hbm, relaxation, tab_sem.at[5]),
    ]

    def tile_of(f, col, row, part=None):
        first, count = (col * n_ty + row) * per_tile, per_tile
        if part is not None:
            count = per_tile // 2
            first = first + part * count
        return gathered[f].at[pl.ds(first, count)]

    def column_of(f, col):
        return gathered[f].at[pl.ds(col * n_ty * per_tile, n_ty * per_tile)]

    barrier = pltpu.get_barrier_semaphore()
    pl.semaphore_signal(barrier, inc=1, device_id={"tx": mate}, device_id_type=MESH)
    for k in range(1, n_ty):
        pl.semaphore_signal(barrier, inc=1, device_id={"ty": (ty + k) % n_ty}, device_id_type=MESH)
    here = (tx * n_ty + ty) * per_tile

    own = [
        pltpu.make_async_copy(fields.at[f, :, pl.ds(b * BS, BS)], gathered[f].at[here + b], own_sem.at[f, b])
        for f in range(n_fields)
        for b in range(per_tile)
    ]
    for copy in own + tabs:
        copy.start()
    pl.semaphore_wait(barrier, n_ty)
    for copy in own:
        copy.wait()

    def to_mate(f, ref):
        return pltpu.make_async_remote_copy(
            src_ref=ref, dst_ref=ref, send_sem=mate_send.at[f], recv_sem=mate_recv.at[f],
            device_id={"tx": mate}, device_id_type=MESH)

    def sign(way):
        return 1 if way == 0 else -1

    def travels(way, h, d):
        return d < depth - 1 or (d == depth - 1 and h == way)

    def ring_copy(f, way, h, d):
        ref = tile_of(f, tx, ring_to_ty(ring - sign(way) * d), h)
        return pltpu.make_async_remote_copy(
            src_ref=ref, dst_ref=ref,
            send_sem=ring_send.at[f], recv_sem=ring_recv.at[f, way, h, d],
            device_id={"ty": toward[way]}, device_id_type=MESH)

    def arrived(f, way, h, d):
        ref = tile_of(f, tx, ring_to_ty(ring - sign(way) * (d + 1)), h)
        pltpu.make_async_remote_copy(
            src_ref=ref, dst_ref=ref, send_sem=ring_send.at[f], recv_sem=ring_recv.at[f, way, h, d],
            device_id={"ty": toward[way]}, device_id_type=MESH).wait_recv()
        return ref

    def stage(g, d):
        for f in range(g * GROUP, (g + 1) * GROUP):
            for h in range(2):
                for way in range(2):
                    came = d > 0 and travels(way, h, d - 1)
                    if came:
                        got = arrived(f, way, h, d - 1)
                    if travels(way, h, d):
                        ring_copy(f, way, h, d).start()
                    if came:
                        to_mate(f, got).start()
            if d == 0:
                to_mate(f, tile_of(f, tx, ty)).start()

    def tendency(g):
        for f in range(g * GROUP, (g + 1) * GROUP):
            for b in range(per_tile):
                span = slice(b * BS, (b + 1) * BS)
                total = coupling[f : f + 1, 0:1].astype(jnp.float32) * gathered[0][here + b].astype(jnp.float32)
                for k in range(1, n_fields):
                    total = total + coupling[f : f + 1, k : k + 1].astype(jnp.float32) * gathered[k][here + b].astype(jnp.float32)
                out[f, :, span] = total

    def upstream(g):
        for f in range(g * GROUP, (g + 1) * GROUP):
            to_mate(f, column_of(f, mate)).wait_recv()
            for j in range(per_tile):
                span = slice(j * BS, (j + 1) * BS)

                first = gathered[f][picks[0, j]].astype(jnp.float32)
                second = gathered[f][picks[1, j]].astype(jnp.float32)
                w = weights[:, span].astype(jnp.float32)
                out[f, :, span] = out[f, :, span] + (w * first + (1.0 - w) * second)
            col_modes = jnp.zeros((rows, 128), jnp.float32)
            for start in range(0, cols, 2 * BS):
                span = slice(start, start + 2 * BS)
                col_modes += jnp.dot(out[f, :, span], col_b[span, :], precision=HI, preferred_element_type=jnp.float32)
            part = jnp.dot(row_bt[...], col_modes, precision=HI, preferred_element_type=jnp.float32)
            modes[g][pl.ds((f - g * GROUP) * 128, 128), :] = part
        swap_copy(g).start()

    half = GROUP * 128 // n_tx
    span_rows = half // n_ty

    def half_copy(src, dst, send, recv):
        return pltpu.make_async_remote_copy(
            src_ref=src, dst_ref=dst, send_sem=send, recv_sem=recv, device_id={"tx": mate}, device_id_type=MESH)

    def swap_copy(g):
        src = modes[g].at[pl.ds(pl.multiple_of(mate * half, 8), half), :]
        return half_copy(src, swapped[g], swap_send.at[g], swap_recv.at[g])

    def back_copy(g):
        ref = ag_bufs[g].at[pl.ds(pl.multiple_of(tx * half, 8), half), :]
        return half_copy(ref, ref, back_send.at[g], back_recv.at[g])

    def rs_copy(g, k):
        there = (ty + k) % n_ty
        return pltpu.make_async_remote_copy(
            src_ref=chip_sums[g].at[pl.ds(pl.multiple_of(there * span_rows, 8), span_rows), :], dst_ref=rs_bufs[g].at[k - 1],
            send_sem=rs_send.at[g], recv_sem=rs_recv.at[g], device_id={"ty": there}, device_id_type=MESH)

    def ag_copy(g, k):
        there = (ty + k) % n_ty
        return pltpu.make_async_remote_copy(
            src_ref=sums[g], dst_ref=ag_bufs[g].at[pl.ds(pl.multiple_of(tx * half + ty * span_rows, 8), span_rows), :],
            send_sem=ag_send.at[g], recv_sem=ag_recv.at[g], device_id={"ty": there}, device_id_type=MESH)

    def scatter(g):
        swap_copy(g).wait_recv()
        chip_sums[g][...] = modes[g][pl.ds(pl.multiple_of(tx * half, 8), half), :] + swapped[g][...]
        for k in range(1, n_ty):
            rs_copy(g, k).start()

    def reduce(g):
        whole = rs_bufs[g]
        half_copy(whole, whole, rs_send.at[g], rs_recv.at[g]).wait_recv()
        mine = chip_sums[g][pl.ds(pl.multiple_of(ty * span_rows, 8), span_rows), :]
        total = mine + jnp.sum(rs_bufs[g][...], axis=0)
        sums[g][...] = total
        for k in range(1, n_ty):
            ag_copy(g, k).start()
        ag_bufs[g][pl.ds(pl.multiple_of(tx * half + ty * span_rows, 8), span_rows), :] = total

    def hand_back(g):
        whole = rs_bufs[g]
        half_copy(whole, whole, ag_send.at[g], ag_recv.at[g]).wait_recv()
        back_copy(g).start()

    def nudge(g):
        ref = ag_bufs[g].at[pl.ds(pl.multiple_of(mate * half, 8), half), :]
        half_copy(ref, ref, back_send.at[g], back_recv.at[g]).wait_recv()
        for f in range(g * GROUP, (g + 1) * GROUP):
            coef = ag_bufs[g][pl.ds((f - g * GROUP) * 128, 128), :]
            term = relaxation[f] * (driver[f] - coef)
            recon = jnp.dot(row_b[...], term, precision=HI, preferred_element_type=jnp.float32)
            for start in range(0, cols, 2 * BS):
                span = slice(start, start + 2 * BS)
                out[f, :, span] += lax.dot_general(
                    recon, col_b[span, :], (((1,), (1,)), ((), ())), precision=HI, preferred_element_type=jnp.float32)

    stage(0, 0)
    for g in range(n_groups):
        tendency(g)
    for copy in tabs:
        copy.wait()
    end = n_groups - 1
    for g in range(end):
        behind = [upstream, scatter, reduce] if g > 0 else []
        for d in range(1, depth):
            stage(g, d)
            if behind:
                behind.pop(0)(g - 1)
        stage(g + 1, 0)
        stage(g, depth)
        if g > 0:
            for step in behind + [hand_back, nudge]:
                step(g - 1)
    for d in range(1, depth):
        stage(end, d)
        if d == 1:
            upstream(end - 1)
    scatter(end - 1)
    stage(end, depth)
    reduce(end - 1)
    upstream(end)
    scatter(end)
    hand_back(end - 1)
    reduce(end)
    nudge(end - 1)
    hand_back(end)
    nudge(end)

    for f in range(n_fields):
        sent = gathered[f].at[pl.ds(0, (n_ty - 1) * per_tile)]
        pltpu.make_async_remote_copy(
            src_ref=sent, dst_ref=sent, send_sem=ring_send.at[f], recv_sem=ring_recv.at[f, 0, 0, 0],
            device_id={"ty": toward[0]}, device_id_type=MESH).wait_send()
        to_mate(f, column_of(f, tx)).wait_send()
    for g in range(n_groups):
        swap_copy(g).wait_send()
        back_copy(g).wait_send()
        whole = rs_bufs[g]
        half_copy(whole, whole, rs_send.at[g], rs_recv.at[g]).wait_send()
        half_copy(whole, whole, ag_send.at[g], ag_recv.at[g]).wait_send()


def ladder(mesh):
    devices = np.asarray(mesh.devices)
    axis = list(mesh.axis_names).index("ty")
    line = np.moveaxis(devices, axis, 0).reshape(devices.shape[axis], -1)[:, 0]
    coords = [getattr(d, "coords", None) for d in line]
    if len(line) != 8 or mesh.shape["tx"] != 2 or any(c is None for c in coords):
        return False
    steps = [[b - a for a, b in zip(coords[0], c)] for c in coords]
    rung, rail = steps[1], steps[2]
    unit = sum(abs(v) for v in rung) == 1 and sum(abs(v) for v in rail) == 1
    return unit and all(
        s == [k // 2 * v + k % 2 * w for v, w in zip(rail, rung)] for k, s in enumerate(steps))


SPLIT = 2
PATTERN = "PQPPQPPQPPQP"
LAUNCH, SECOND, COLLECT, ANSWER, FINISH = 3, 1, 2, 3, 5
ADDS = ((1, 2, 1, 1), (1, 2))
GROUPS = (5, 1)


def ladder_plan(n_fields, rows):
    pieces = SPLIT if rows % (16 * SPLIT) == 0 else 1
    size = rows // pieces
    spots = [(f, r) for f in range(n_fields) for r in range(0, rows, size)]
    chunks = [(f, r, size, PATTERN[k % len(PATTERN)]) for k, (f, r) in enumerate(spots)]
    counts = GROUPS if sum(GROUPS) == n_fields else (1,) * n_fields
    ends = [sum(counts[: k + 1]) for k in range(len(counts))]
    groups = [tuple(range(e - n, e)) for e, n in zip(ends, counts)]
    return tuple(chunks), tuple(groups)


def ladder_kernel(
    n_ty, n_tx, chunks, groups,
    fields, weights_hbm, tile_s, block_s, coupling, driver_hbm, relaxation_hbm, row_tab, row_tab_t, col_tab,
    result, *scratch,
):
    out, out_sem, *scratch = scratch
    n_fields, rows, cols = fields.shape
    n_chunks, n_groups = len(chunks), len(groups)
    gathered, asked, slots = (scratch[k * n_chunks : (k + 1) * n_chunks] for k in range(3))
    scratch = scratch[3 * n_chunks :]
    (modes, swapped, chip_sums, rs_bufs, sums, ag_bufs) = (
        scratch[k * n_groups : (k + 1) * n_groups] for k in range(6))
    (row_b, row_bt, col_b, weights, driver, relaxation, mine, rung_tile, rung_block, outer_tile, outer_block,
     tab_sem, own_sem, mine_sem, want_send, want_recv, sent, recv, mate_send, mate_recv,
     rs_send, rs_recv, ag_send, ag_recv, swap_send, swap_recv, back_send, back_recv) = scratch[6 * n_groups :]
    per_tile = cols // BS
    n_z = n_ty // 2
    n_ask = 2 * per_tile
    ty = lax.axis_index("ty")
    tx = lax.axis_index("tx")
    mate = 1 - tx
    z, y = ty // 2, ty % 2
    far_y = 1 - y
    left = z < n_z // 2
    end = (z == 0) | (z == n_z - 1)
    inner = jnp.logical_not(end)
    z_end = jnp.where(left, 0, n_z - 1)
    z_in = jnp.where(left, 1, n_z - 2)
    far_end, far_in = n_z - 1 - z_end, n_z - 1 - z_in
    rung = 2 * z + far_y
    across = 2 * far_in + y
    outer = 2 * z_end + y
    inward = 2 * z_in + y

    def copy_to(src, dst, send, got, where):
        return pltpu.make_async_remote_copy(
            src_ref=src, dst_ref=dst, send_sem=send, recv_sem=got, device_id=where, device_id_type=MESH)

    def tile(c, zz, yy, part=None, col=None):
        first, count = ((tx if col is None else col) * n_ty + yy * n_z + zz) * per_tile, per_tile
        if part is not None:
            count = per_tile // 2
            first = first + part * count
        return gathered[c].at[pl.ds(first, count)]

    def rail(c, col):
        return gathered[c].at[pl.ds((col * n_ty + y * n_z) * per_tile, n_z * per_tile)]

    def column(c, col):
        return gathered[c].at[pl.ds(col * n_ty * per_tile, n_ty * per_tile)]

    def send(c, ref, there, kind):
        copy_to(ref, ref, sent.at[c], recv.at[c, kind], {"ty": there}).start()

    def take(c, ref, kind):
        copy_to(ref, ref, sent.at[c], recv.at[c, kind], {"ty": rung}).wait_recv()

    def to_mate(c, ref):
        return copy_to(ref, ref, mate_send.at[c], mate_recv.at[c], {"tx": mate})

    E_OWN, E_FAR, I_ACROSS, E_ACROSS, I_PART, OWN_RUNG, E_RUNG, I_REST, ASKED = range(9)

    tabs = [
        pltpu.make_async_copy(row_tab.at[pl.ds(ty * rows, rows), :], row_b, tab_sem.at[0]),
        pltpu.make_async_copy(row_tab_t.at[:, pl.ds(pl.multiple_of(ty * rows, 128), rows)], row_bt, tab_sem.at[1]),
        pltpu.make_async_copy(col_tab.at[pl.ds(tx * cols, cols), :], col_b, tab_sem.at[2]),
        pltpu.make_async_copy(weights_hbm, weights, tab_sem.at[3]),
        pltpu.make_async_copy(driver_hbm, driver, tab_sem.at[4]),
        pltpu.make_async_copy(relaxation_hbm, relaxation, tab_sem.at[5]),
    ]

    barrier = pltpu.get_barrier_semaphore()
    pl.semaphore_signal(barrier, inc=1, device_id={"tx": mate}, device_id_type=MESH)
    pl.semaphore_signal(barrier, inc=1, device_id={"ty": rung}, device_id_type=MESH)

    @pl.when(inner)
    def _():
        pl.semaphore_signal(barrier, inc=1, device_id={"ty": across}, device_id_type=MESH)
        pl.semaphore_signal(barrier, inc=1, device_id={"ty": outer}, device_id_type=MESH)

    @pl.when(end)
    def _():
        pl.semaphore_signal(barrier, inc=1, device_id={"ty": inward}, device_id_type=MESH)
    here = (tx * n_ty + y * n_z + z) * per_tile
    own = [
        [pltpu.make_async_copy(fields.at[f, pl.ds(r0, nr), pl.ds(b * BS, BS)], gathered[c].at[here + b], own_sem.at[c, b])
         for b in range(per_tile)]
        for c, (f, r0, nr, _) in enumerate(chunks)
    ]
    mine_copy = pltpu.make_async_copy(fields, mine, mine_sem)
    for copies in own:
        for copy in copies:
            copy.start()
    for copy in [mine_copy] + tabs:
        copy.start()

    @pl.when(inner)
    def _():
        pl.semaphore_wait(barrier, 4)

    @pl.when(end)
    def _():
        pl.semaphore_wait(barrier, 3)

    want = [
        (copy_to(tile_s, rung_tile, want_send.at[0], want_recv.at[0], {"ty": rung}),
         copy_to(block_s, rung_block, want_send.at[1], want_recv.at[1], {"ty": rung})),
        (copy_to(tile_s, outer_tile, want_send.at[2], want_recv.at[2], {"ty": inward}),
         copy_to(block_s, outer_block, want_send.at[3], want_recv.at[3], {"ty": inward})),
    ]
    for copy in want[0]:
        copy.start()

    @pl.when(end)
    def _():
        for copy in want[1]:
            copy.start()

    def spot(tiles, blocks, s, j):
        t = tiles[s, j]
        row, col = lax.div(t, n_tx), lax.rem(t, n_tx)
        row_z, row_y = lax.div(row, 2), lax.rem(row, 2)
        return col, row_z, row_y, blocks[s, j]

    def place(col, row_z, row_y, block):
        return (col * n_ty + row_y * n_z + row_z) * per_tile + block

    def launch(c):
        for copy in own[c]:
            copy.wait()
        ref = tile(c, z, y)
        if chunks[c][3] == "P":
            @pl.when(inner)
            def _():
                send(c, ref, rung, OWN_RUNG)
                send(c, ref, across, I_ACROSS)
                to_mate(c, ref).start()

            @pl.when(end)
            def _():
                send(c, ref, rung, OWN_RUNG)
                send(c, ref, inward, E_OWN)
        else:
            @pl.when(inner)
            def _():
                send(c, ref, across, I_ACROSS)
                send(c, ref, outer, E_OWN)

            @pl.when(end)
            def _():
                send(c, ref, inward, E_OWN)
            to_mate(c, ref).start()

    def first_hop(c):
        if chunks[c][3] == "P":
            @pl.when(inner)
            def _():
                ref = tile(c, z_end, y)
                take(c, ref, E_OWN)
                send(c, ref, across, E_ACROSS)
                to_mate(c, ref).start()
                ref = tile(c, z, far_y)
                take(c, ref, OWN_RUNG)
                send(c, tile(c, z, far_y, 0), across, I_PART)
                to_mate(c, ref).start()
                ref = tile(c, far_in, y)
                take(c, ref, I_ACROSS)
                send(c, tile(c, far_in, y, 1), rung, I_REST)
                to_mate(c, ref).start()

            @pl.when(end)
            def _():
                ref = tile(c, z, far_y)
                take(c, ref, OWN_RUNG)
                send(c, ref, inward, E_FAR)
        else:
            @pl.when(inner)
            def _():
                ref = tile(c, z_end, y)
                take(c, ref, E_OWN)
                send(c, ref, across, E_ACROSS)
                to_mate(c, ref).start()
                ref = tile(c, far_in, y)
                take(c, ref, I_ACROSS)
                send(c, ref, outer, I_ACROSS)
                to_mate(c, ref).start()

            @pl.when(end)
            def _():
                ref = tile(c, z_in, y)
                take(c, ref, E_OWN)
                to_mate(c, ref).start()

    def second_hop(c):
        if chunks[c][3] == "P":
            @pl.when(inner)
            def _():
                ref = tile(c, far_end, y)
                take(c, ref, E_ACROSS)
                send(c, ref, rung, E_RUNG)
                to_mate(c, ref).start()
                ref = tile(c, z_end, far_y)
                take(c, ref, E_FAR)
                to_mate(c, ref).start()
        else:
            @pl.when(inner)
            def _():
                ref = tile(c, far_end, y)
                take(c, ref, E_ACROSS)
                send(c, ref, outer, E_ACROSS)
                to_mate(c, ref).start()

            @pl.when(end)
            def _():
                ref = tile(c, far_in, y)
                take(c, ref, I_ACROSS)
                to_mate(c, ref).start()

    def collect(c):
        if chunks[c][3] == "P":
            @pl.when(inner)
            def _():
                take(c, tile(c, far_in, far_y, 0), I_PART)
                take(c, tile(c, far_in, far_y, 1), I_REST)
                to_mate(c, tile(c, far_in, far_y)).start()
                ref = tile(c, far_end, far_y)
                take(c, ref, E_RUNG)
                to_mate(c, ref).start()
        else:
            @pl.when(end)
            def _():
                ref = tile(c, far_end, y)
                take(c, ref, E_ACROSS)
                to_mate(c, ref).start()

    def answer(c):
        if chunks[c][3] == "P":
            @pl.when(inner)
            def _():
                to_mate(c, column(c, mate)).wait_recv()
                for s in range(2):
                    for j in range(per_tile):
                        col, row_z, row_y, block = spot(outer_tile, outer_block, s, j)
                        asked[c][s * per_tile + j] = gathered[c][place(col, row_z, row_y, block)]
                copy_to(asked[c], slots[c], sent.at[c], recv.at[c, ASKED], {"ty": outer}).start()
        else:
            to_mate(c, rail(c, mate)).wait_recv()
            for s in range(2):
                for j in range(per_tile):
                    col, row_z, row_y, block = spot(rung_tile, rung_block, s, j)
                    asked[c][s * per_tile + j] = gathered[c][place(col, row_z, y, block)]
            copy_to(asked[c], slots[c], sent.at[c], recv.at[c, ASKED], {"ty": rung}).start()

    def blend(c):
        f, r0, nr, mode = chunks[c]
        whole = copy_to(asked[c], slots[c], sent.at[c], recv.at[c, ASKED], {"ty": rung})
        if mode == "P":
            @pl.when(end)
            def _():
                whole.wait_recv()
        else:
            whole.wait_recv()

        def source(s, j):
            col, row_z, row_y, block = spot(tile_s, block_s, s, j)
            if mode == "P":
                here_too = inner
                at = place(col, row_z, row_y, block)
            else:
                here_too = row_y == y
                at = place(col, row_z, y, block)
            return jnp.where(here_too, gathered[c][at].astype(jnp.float32), slots[c][s * per_tile + j].astype(jnp.float32))

        for j in range(per_tile):
            span = slice(j * BS, (j + 1) * BS)
            w = weights[r0 : r0 + nr, span].astype(jnp.float32)
            out[f, r0 : r0 + nr, span] = out[f, r0 : r0 + nr, span] + (w * source(0, j) + (1.0 - w) * source(1, j))

    def tendency(f):
        for b in range(per_tile):
            span = slice(b * BS, (b + 1) * BS)
            total = coupling[f : f + 1, 0:1].astype(jnp.float32) * mine[0, :, span].astype(jnp.float32)
            for k in range(1, n_fields):
                total = total + coupling[f : f + 1, k : k + 1].astype(jnp.float32) * mine[k, :, span].astype(jnp.float32)
            out[f, :, span] = total

    def project(g, f):
        col_modes = jnp.zeros((rows, 128), jnp.float32)
        for start in range(0, cols, 2 * BS):
            span = slice(start, start + 2 * BS)
            col_modes += jnp.dot(out[f, :, span], col_b[span, :], precision=HI, preferred_element_type=jnp.float32)
        part = jnp.dot(row_bt[...], col_modes, precision=HI, preferred_element_type=jnp.float32)
        modes[g][pl.ds((f - groups[g][0]) * 128, 128), :] = part
        if f == groups[g][-1]:
            if g in direct:
                spread(g)
            else:
                swap_copy(g).start()

    direct = (n_groups - 1,)

    def sizes(g):
        half = len(groups[g]) * 128 // n_tx
        return half, half // n_ty

    def rows_of(ref, first, count):
        return ref.at[pl.ds(pl.multiple_of(first, 8), count), :]

    def swap_copy(g):
        half, _ = sizes(g)
        return copy_to(rows_of(modes[g], mate * half, half), swapped[g], swap_send.at[g], swap_recv.at[g], {"tx": mate})

    def back_copy(g):
        half, _ = sizes(g)
        ref = rows_of(ag_bufs[g], tx * half, half)
        return copy_to(ref, ref, back_send.at[g], back_recv.at[g], {"tx": mate})

    def rs_copy(g, k):
        _, span = sizes(g)
        there = (ty + k) % n_ty
        src = rows_of(chip_sums[g], there * span, span)
        return copy_to(src, rs_bufs[g].at[k - 1], rs_send.at[g], rs_recv.at[g], {"ty": there})

    def ag_copy(g, k):
        half, span = sizes(g)
        dst = rows_of(ag_bufs[g], tx * half + ty * span, span)
        return copy_to(sums[g], dst, ag_send.at[g], ag_recv.at[g], {"ty": (ty + k) % n_ty})

    def scatter(g):
        half, _ = sizes(g)
        swap_copy(g).wait_recv()
        chip_sums[g][...] = modes[g][pl.ds(pl.multiple_of(tx * half, 8), half), :] + swapped[g][...]
        for k in range(1, n_ty):
            rs_copy(g, k).start()

    def reduce(g):
        half, span = sizes(g)
        whole = rs_bufs[g]
        copy_to(whole, whole, rs_send.at[g], rs_recv.at[g], {"tx": mate}).wait_recv()
        total = chip_sums[g][pl.ds(pl.multiple_of(ty * span, 8), span), :] + jnp.sum(rs_bufs[g][...], axis=0)
        sums[g][...] = total
        for k in range(1, n_ty):
            ag_copy(g, k).start()
        ag_bufs[g][pl.ds(pl.multiple_of(tx * half + ty * span, 8), span), :] = total

    def hand_back(g):
        whole = rs_bufs[g]
        copy_to(whole, whole, ag_send.at[g], ag_recv.at[g], {"tx": mate}).wait_recv()
        back_copy(g).start()

    def nudge(g):
        half, _ = sizes(g)
        ref = rows_of(ag_bufs[g], mate * half, half)
        copy_to(ref, ref, back_send.at[g], back_recv.at[g], {"tx": mate}).wait_recv()
        correct(g)

    def correct(g):
        for f in groups[g]:
            coef = ag_bufs[g][pl.ds((f - groups[g][0]) * 128, 128), :]
            term = relaxation[f] * (driver[f] - coef)
            recon = jnp.dot(row_b[...], term, precision=HI, preferred_element_type=jnp.float32)
            for start in range(0, cols, 2 * BS):
                span = slice(start, start + 2 * BS)
                out[f, :, span] += lax.dot_general(
                    recon, col_b[span, :], (((1,), (1,)), ((), ())), precision=HI, preferred_element_type=jnp.float32)
            pltpu.make_async_copy(out.at[f], result.at[f], out_sem.at[f]).start()

    n_own = n_ty * n_tx // 2

    def relations():
        for dz in range(2):
            for dy in range(2):
                for dt in range(2):
                    yield dz * 4 + dy * 2 + dt, (z_in, far_in)[dz], (z_end, far_end)[dz], (y, far_y)[dy], (tx, mate)[dt]

    def owner_rows(g, zz, yy, tt):
        span = len(groups[g]) * 128 // n_own
        return ((zz - 1) * 4 + yy * 2 + tt) * span, span

    def spread_copy(g, slot, zz, yy, tt):
        src = rows_of(modes[g], *owner_rows(g, zz, yy, tt))
        return copy_to(src, rs_bufs[g].at[slot], rs_send.at[g], rs_recv.at[g], {"ty": 2 * zz + yy, "tx": tt})

    def spread(g):
        @pl.when(inner)
        def _():
            for k, zz, _, yy, tt in relations():
                if k:
                    spread_copy(g, k, zz, yy, tt).start()

        @pl.when(end)
        def _():
            for k, zz, _, yy, tt in relations():
                spread_copy(g, n_own + k, zz, yy, tt).start()

    def slices(g, count):
        ref = rs_bufs[g].at[pl.ds(0, count)]
        return copy_to(ref, ref, rs_send.at[g], rs_recv.at[g], {"tx": mate})

    def answers(g, count):
        ref = rs_bufs[g].at[pl.ds(0, count)]
        return copy_to(ref, ref, ag_send.at[g], ag_recv.at[g], {"tx": mate})

    def settle(g):
        @pl.when(inner)
        def _():
            slices(g, 2 * n_own - 1).wait_recv()
            first, span = owner_rows(g, z, y, tx)
            total = modes[g][pl.ds(pl.multiple_of(first, 8), span), :] + jnp.sum(rs_bufs[g][1:], axis=0)
            sums[g][...] = total
            dst = rows_of(ag_bufs[g], first, span)
            for k, zz, ze, yy, tt in relations():
                copy_to(sums[g], dst, ag_send.at[g], ag_recv.at[g], {"ty": 2 * ze + yy, "tx": tt}).start()
                if k:
                    copy_to(sums[g], dst, ag_send.at[g], ag_recv.at[g], {"ty": 2 * zz + yy, "tx": tt}).start()
            ag_bufs[g][pl.ds(pl.multiple_of(first, 8), span), :] = total

    def nudge_direct(g):
        @pl.when(inner)
        def _():
            answers(g, n_own - 1).wait_recv()

        @pl.when(end)
        def _():
            answers(g, n_own).wait_recv()
        correct(g)

    last_chunk = {f: c for c, (f, _, _, _) in enumerate(chunks)}
    group_of = {f: g for g, fs in enumerate(groups) for f in fs}
    todo = {}

    def finish(c, k):
        blend(c)
        f = chunks[c][0]
        if last_chunk[f] == c:
            g = group_of[f]
            project(g, f)
            if f == groups[g][-1]:
                due = k
                steps = (settle, nudge_direct) if g in direct else (scatter, reduce, hand_back, nudge)
                for step, gap in zip(steps, ADDS[g]):
                    due += gap
                    todo.setdefault(due, []).append((step, g))

    started = 0
    while started < min(LAUNCH, n_chunks):
        launch(started)
        started += 1
    mine_copy.wait()
    fresh = list(range(n_fields))
    tendency(fresh.pop(0))
    k = 0
    while k < n_chunks + FINISH or todo:
        if k == 1:
            for copy in tabs:
                copy.wait()
            for copy in want[0]:
                copy.wait_recv()

            @pl.when(inner)
            def _():
                for copy in want[1]:
                    copy.wait_recv()
        if k < n_chunks:
            first_hop(k)
        if started < n_chunks:
            launch(started)
            started += 1
        if 0 <= k - SECOND < n_chunks:
            second_hop(k - SECOND)
        if 0 <= k - COLLECT < n_chunks:
            collect(k - COLLECT)
        if 0 <= k - ANSWER < n_chunks:
            answer(k - ANSWER)
        if fresh:
            tendency(fresh.pop(0))
        for step, g in todo.pop(k, ()):
            step(g)
        if 0 <= k - FINISH < n_chunks:
            finish(k - FINISH, k)
        k += 1

    for c in range(n_chunks):
        mode = chunks[c][3]

        @pl.when(inner)
        def _():
            ref = gathered[c].at[pl.ds(0, 7 * per_tile)]
            copy_to(ref, ref, sent.at[c], recv.at[c, 0], {"ty": rung}).wait_send()
            if mode == "P":
                to_mate(c, column(c, tx)).wait_send()

        @pl.when(end)
        def _():
            ref = gathered[c].at[pl.ds(0, 3 * per_tile)]
            copy_to(ref, ref, sent.at[c], recv.at[c, 0], {"ty": rung}).wait_send()

        if mode == "Q":
            to_mate(c, rail(c, tx)).wait_send()
    for f in range(n_fields):
        pltpu.make_async_copy(out.at[f], result.at[f], out_sem.at[f]).wait()
    for copy in want[0]:
        copy.wait_send()

    @pl.when(end)
    def _():
        for copy in want[1]:
            copy.wait_send()
    for g in range(n_groups):
        if g in direct:
            @pl.when(inner)
            def _():
                slices(g, n_own - 1).wait_send()
                answers(g, 2 * n_own - 1).wait_send()

            @pl.when(end)
            def _():
                slices(g, n_own).wait_send()
        else:
            swap_copy(g).wait_send()
            back_copy(g).wait_send()
            whole = rs_bufs[g]
            copy_to(whole, whole, rs_send.at[g], rs_recv.at[g], {"tx": mate}).wait_send()
            copy_to(whole, whole, ag_send.at[g], ag_recv.at[g], {"tx": mate}).wait_send()


def ladder_call(
    n_ty, n_tx, fields, weights, tile, block, coupling, driver, relaxation, row_tab, row_tab_t, col_tab,
):
    n_fields, rows, cols = fields.shape
    chunks, groups = ladder_plan(n_fields, rows)
    n_chunks, n_groups = len(chunks), len(groups)
    per_tile = cols // BS
    vmem = pl.BlockSpec(memory_space=pltpu.VMEM)
    smem = pl.BlockSpec(memory_space=pltpu.SMEM)
    hbm = pl.BlockSpec(memory_space=pltpu.HBM)
    dma = pltpu.SemaphoreType.DMA
    halves = [len(g) * 128 // n_tx for g in groups]
    asks = pltpu.SMEM((2, per_tile), jnp.int32)
    scratch = (
        [pltpu.VMEM((n_fields, rows, cols), jnp.float32), dma((n_fields,))]
        + [pltpu.VMEM((n_ty * n_tx * per_tile, c[2], BS), jnp.bfloat16) for c in chunks]
        + [pltpu.VMEM((2 * per_tile, c[2], BS), jnp.bfloat16) for c in chunks] * 2
        + [pltpu.VMEM((len(g) * 128, 128), jnp.float32) for g in groups]
        + [pltpu.VMEM((h, 128), jnp.float32) for h in halves] * 2
        + [pltpu.VMEM((n_ty - 1, h // n_ty, 128), jnp.float32) for h in halves[:-1]]
        + [pltpu.VMEM((n_ty * n_tx, 2 * halves[-1] // n_ty, 128), jnp.float32)]
        + [pltpu.VMEM((h // n_ty, 128), jnp.float32) for h in halves[:-1]]
        + [pltpu.VMEM((2 * halves[-1] // n_ty, 128), jnp.float32)]
        + [pltpu.VMEM((len(g) * 128, 128), jnp.float32) for g in groups]
        + [
            pltpu.VMEM((rows, 128), jnp.float32),
            pltpu.VMEM((128, rows), jnp.float32),
            pltpu.VMEM((cols, 128), jnp.float32),
            pltpu.VMEM((rows, cols), jnp.bfloat16),
            pltpu.VMEM(driver.shape, jnp.float32),
            pltpu.VMEM(relaxation.shape, jnp.float32),
            pltpu.VMEM(fields.shape, jnp.bfloat16),
            asks, asks, asks, asks,
            dma((6,)),
            dma((n_chunks, per_tile)),
            dma,
            dma((4,)),
            dma((4,)),
            dma((n_chunks,)),
            dma((n_chunks, 9)),
            dma((n_chunks,)),
            dma((n_chunks,)),
            *[dma((n_groups,))] * 8,
        ]
    )
    return pl.pallas_call(
        functools.partial(ladder_kernel, n_ty, n_tx, chunks, groups),
        out_shape=jax.ShapeDtypeStruct((n_fields, rows, cols), jnp.float32),
        in_specs=[hbm, hbm, smem, smem, vmem, hbm, hbm, hbm, hbm, hbm],
        out_specs=hbm,
        scratch_shapes=scratch,
        compiler_params=pltpu.CompilerParams(
            collective_id=0, has_side_effects=True, vmem_limit_bytes=67043328
        ),
        name="remap_ladder",
    )(fields, weights, tile, block, coupling, driver, relaxation, row_tab, row_tab_t, col_tab)


def solution(mesh):
    n_ty, n_tx = mesh.shape["ty"], mesh.shape["tx"]
    snake = two_lines(mesh)
    rungs = ladder(mesh)

    def body(fields, weights, source_tile, source_block, coupling, driver, relaxation):
        n_fields, rows, cols = fields.shape
        n_groups = n_fields // GROUP
        n_dev = n_ty * n_tx
        half = GROUP * 128 // n_tx
        span_rows = half // n_ty
        row_np, col_np = wave_table(rows * n_ty), wave_table(cols * n_tx)
        row_tab, row_tab_t = jnp.asarray(row_np), jnp.asarray(np.ascontiguousarray(row_np.T))
        if row_np.shape == col_np.shape:
            col_tab = row_tab
        else:
            col_tab = jnp.asarray(col_np)
        tile = jnp.transpose(source_tile, (0, 2, 1))[0]
        block = jnp.transpose(source_block, (0, 2, 1))[0]
        if rungs:
            return ladder_call(
                n_ty, n_tx, fields, weights, tile, block, coupling, driver, relaxation, row_tab, row_tab_t, col_tab)
        picks = (tile % n_tx * n_ty + tile // n_tx) * (cols // BS) + block
        vmem = pl.BlockSpec(memory_space=pltpu.VMEM)
        smem = pl.BlockSpec(memory_space=pltpu.SMEM)
        hbm = pl.BlockSpec(memory_space=pltpu.HBM)
        dma = pltpu.SemaphoreType.DMA
        scratch = (
            [pltpu.VMEM((n_dev * (cols // BS), BS, BS), jnp.bfloat16)] * n_fields
            + [pltpu.VMEM((GROUP * 128, 128), jnp.float32)] * n_groups
            + [pltpu.VMEM((half, 128), jnp.float32)] * (2 * n_groups)
            + [pltpu.VMEM((n_ty - 1, span_rows, 128), jnp.float32)] * n_groups
            + [pltpu.VMEM((span_rows, 128), jnp.float32)] * n_groups
            + [pltpu.VMEM((GROUP * 128, 128), jnp.float32)] * n_groups
            + [
                pltpu.VMEM((rows, 128), jnp.float32),
                pltpu.VMEM((128, rows), jnp.float32),
                pltpu.VMEM((cols, 128), jnp.float32),
                pltpu.VMEM((rows, cols), jnp.bfloat16),
                pltpu.VMEM(driver.shape, jnp.float32),
                pltpu.VMEM(relaxation.shape, jnp.float32),
                dma((6,)),
                dma((n_fields, cols // BS)),
                dma((n_fields,)),
                dma((n_fields, 2, 2, n_ty // 2)),
                dma((n_fields,)),
                dma((n_fields,)),
                *[dma((n_groups,))] * 8,
            ]
        )
        return pl.pallas_call(
            functools.partial(ring_kernel, n_ty, n_tx, snake),
            out_shape=jax.ShapeDtypeStruct((n_fields, rows, cols), jnp.float32),
            in_specs=[hbm, hbm, smem, vmem, hbm, hbm, hbm, hbm, hbm],
            out_specs=vmem,
            scratch_shapes=scratch,
            compiler_params=pltpu.CompilerParams(
                collective_id=0, has_side_effects=True, vmem_limit_bytes=67043328
            ),
            name="remap_nudge",
        )(fields, weights, picks, coupling, driver, relaxation, row_tab, row_tab_t, col_tab)

    in_specs = (
        P(None, ("groups", "ty"), "tx"),
        P(("groups", "ty"), "tx"),
        P(("groups", "ty"), "tx", None),
        P(("groups", "ty"), "tx", None),
        P(),
        P(),
        P(),
    )
    out_specs = P(None, ("groups", "ty"), "tx")
    return jax.shard_map(body, mesh=mesh, in_specs=in_specs, out_specs=out_specs, check_vma=False)
```
